32 devices in a mesh: dp: 16 (over z, y, x), mp: 2 (over core).
Axes of the slice: x: 2, y: 2, z: 4, core: 2. Of those that a mesh axis runs over, the one named last changes fastest.
Arguments:
- hidden: bfloat16 [4096, 8192], P('dp', 'mp'), may hold values from -6 to 6
- w_key: bfloat16 [8192, 1024], P('mp', 'dp'), may hold values from -0.0625 to 0.0625
- w_value: bfloat16 [8192, 1024], P('mp', 'dp'), may hold values from -0.0625 to 0.0625
- queries: bfloat16 [4096, 8192], P('dp', 'mp'), may hold values from -150 to 150
- lengths: int32 [16], replicated, may hold values from 1 to 512, as said below
- seq_of_slot: int32 [32], replicated, may hold values from 0 to 15, as said below
- pos_of_slot: int32 [32], replicated, may hold values from 0 to 3, as said below
Outputs:
- context: bfloat16 [4096, 8192], P('dp', 'mp')
- key_cache: bfloat16 [16, 512, 1024], P('dp', None, 'mp')
- value_cache: bfloat16 [16, 512, 1024], P('dp', None, 'mp')
The draws below stay inside these ranges and needn't reach their ends.
Inputs may be any that keep to these rules, and one draw needn't show every extreme that they name: Sequence q has ceil(lengths[q] / 128) blocks, 1 to 4; some sequence has 4 full blocks. `seq_of_slot`: slots 2 i and 2 i + 1 belong to replica i. Every block of every sequence stands in exactly one slot. The blocks of one sequence stand on different replicas; the two slots of a replica hold blocks of different sequences; and for any two replicas A and B, at most one block on A is an earlier block of the same sequence as some block on B. `pos_of_slot`: given with seq_of_slot: the block index, from 0, of the block in each slot.
All inputs are finite; a program needn't handle non-finite values.
Results may differ from the reference program's by a relative error of at most 0.011.
Values may be sent and summed in bfloat16 or wider, within the bound.
A program may use at most 128 MiB of HBM per device.

```python
import math
import jax
import jax.numpy as jnp
from jax import lax

D = 8192
HQ = 64
KVH = 8
HD = 128
BLOCK = 128
MAXB = 4
SEQS = 16
TOKENS = 4096


def layout(key):
    total_seqs = SEQS
    groups = total_seqs // 4
    patterns = jnp.array([[4, 1, 1, 2], [3, 3, 1, 1], [2, 2, 2, 2], [4, 2, 1, 1], [3, 2, 2, 1], [1, 1, 3, 3], [2, 3, 1, 2]], jnp.int32)
    chosen = jax.random.randint(jax.random.fold_in(key, 101), (groups,), 0, 7)
    chosen = chosen.at[0].set(0)
    ranking = jax.random.randint(jax.random.fold_in(key, 102), (groups, 4), 0, 1 << 20) * 4 + jnp.arange(4, dtype=jnp.int32)[None, :]
    ordering = jnp.argsort(ranking, axis=1)
    counts = jnp.take_along_axis(patterns[chosen], ordering, axis=1).reshape(total_seqs)
    starts = jnp.cumsum(counts) - counts
    listed = jnp.arange(2 * total_seqs, dtype=jnp.int32)
    seq_listed = jnp.sum((starts[None, :] <= listed[:, None]).astype(jnp.int32), axis=1) - 1
    pos_listed = listed - starts[seq_listed]
    front_half = listed < total_seqs
    column = jnp.where(front_half, listed, (2 * total_seqs - listed) % total_seqs)
    shuffle = jax.random.permutation(jax.random.fold_in(key, 103), total_seqs)
    slot_index = shuffle[column] * 2 + jnp.where(front_half, 0, 1)
    seq_slots = jnp.zeros((2 * total_seqs,), jnp.int32).at[slot_index].set(seq_listed)
    pos_slots = jnp.zeros((2 * total_seqs,), jnp.int32).at[slot_index].set(pos_listed)
    tail_fill = jax.random.randint(jax.random.fold_in(key, 104), (total_seqs,), 1, BLOCK + 1)
    longest = jnp.argmax(counts == 4)
    tail_fill = tail_fill.at[longest].set(BLOCK)
    lengths = (counts - 1) * BLOCK + tail_fill
    return (lengths.astype(jnp.int32), seq_slots.astype(jnp.int32), pos_slots.astype(jnp.int32))


def draw_lengths(key, part):
    return layout(key)[0]


def draw_seq_of_slot(key, part):
    return layout(key)[1]


def draw_pos_of_slot(key, part):
    return layout(key)[2]


def draw_queries(key, part):
    shape = (TOKENS, HQ * HD)
    values = jnp.clip(jax.random.normal(jax.random.fold_in(key, 204), shape, jnp.float32), -6.0, 6.0)
    return values.astype(jnp.bfloat16)


def shard_levels(key, shape, shards, least, high):
    factor_of = 1.0
    for position, parts in shards:
        steps = jax.random.uniform(jax.random.fold_in(jax.random.fold_in(key, 6), position), (parts,), jnp.float32, least / len(shards), high / len(shards))
        factor_of = factor_of * jnp.repeat(jnp.exp(steps), shape[position] // parts).reshape((-1,) + (1,) * (len(shape) - 1 - position))
    return factor_of


def bell_draw(own_key, dims, deviation, most, cuts=(), kind=jnp.bfloat16):
    result = jax.random.normal(own_key, dims, jnp.float32) * deviation
    if len(cuts) > 0:
        result = shard_levels(own_key, dims, cuts, -0.22, 0.18) * result
    return jnp.clip(result, min=-most, max=most).astype(kind)


def setup_inputs(seed: int = 0) -> dict:
    seeds = jax.random.split(jax.random.key(seed), 8)
    return {
        "hidden": bell_draw(seeds[0], (TOKENS, D), 1.0, 6.0, ((0, 16), (1, 2))),
        "w_key": bell_draw(seeds[1], (D, KVH * HD), D ** -0.5, 0.0625, ((0, 2), (1, 16))),
        "w_value": bell_draw(seeds[2], (D, KVH * HD), D ** -0.5, 0.0625, ((0, 2), (1, 16))),
        "queries": draw_queries(jax.random.fold_in(seeds[7], 71), 0),
        "lengths": draw_lengths(jax.random.fold_in(seeds[7], 71), 0),
        "seq_of_slot": draw_seq_of_slot(jax.random.fold_in(seeds[7], 71), 0),
        "pos_of_slot": draw_pos_of_slot(jax.random.fold_in(seeds[7], 71), 0),
    }


def rotate(field, positions):
    halfway = field.shape[-1] // 2
    indices = jnp.arange(halfway, dtype=jnp.float32)
    frequency = jnp.exp(-(2.0 * indices / field.shape[-1]) * math.log(500000.0))
    angles = positions[:, None] * frequency[None, :]
    cosines = jnp.cos(angles)[:, None, :]
    sines = jnp.sin(angles)[:, None, :]
    front = field[..., :halfway]
    back = field[..., halfway:]
    return jnp.concatenate([front * cosines - back * sines, back * cosines + front * sines], axis=-1)

def reference(hidden, w_key, w_value, queries, lengths, seq_of_slot, pos_of_slot):
    total = hidden.shape[0]
    slot_count = seq_of_slot.shape[0]
    width = KVH * HD
    key_raw = jnp.dot(hidden, w_key, preferred_element_type=jnp.float32)
    value_rows = jnp.dot(hidden, w_value, preferred_element_type=jnp.float32).astype(jnp.bfloat16)
    rows = jnp.arange(total, dtype=jnp.int32)
    positions = pos_of_slot[rows // BLOCK] * BLOCK + rows % BLOCK
    key_rows = rotate(key_raw.reshape(total, KVH, HD), positions.astype(jnp.float32)).reshape(total, width).astype(jnp.bfloat16)
    slot_ids = jnp.arange(slot_count, dtype=jnp.int32)
    blocks = jnp.arange(MAXB, dtype=jnp.int32)
    sequences = jnp.arange(SEQS, dtype=jnp.int32)
    match = (seq_of_slot[None, None, :] == sequences[:, None, None]) & (pos_of_slot[None, None, :] == blocks[None, :, None])
    source = lax.optimization_barrier(jnp.sum(jnp.where(match, slot_ids[None, None, :], 0), axis=2)).astype(jnp.int32)
    span = MAXB * BLOCK
    cached = jnp.arange(span, dtype=jnp.int32)
    inside = cached[None, :] < lengths[:, None]

    def assemble(rows_all):
        blocked = rows_all.reshape(slot_count, BLOCK, width)[source].reshape(SEQS, span, width)
        return jnp.where(inside[:, :, None], blocked, jnp.zeros_like(blocked))
    key_cache = assemble(key_rows)
    value_cache = assemble(value_rows)
    ratio = HQ // KVH
    query_blocks = queries.reshape(slot_count, BLOCK, KVH, ratio, HD)
    offsets = jnp.arange(BLOCK, dtype=jnp.int32)

    def attend(slot_index):
        sequence = seq_of_slot[slot_index]
        length = lengths[sequence]
        query_pos = pos_of_slot[slot_index] * BLOCK + offsets
        allowed = (cached[None, :] <= query_pos[:, None]) & (cached[None, :] < length)
        key_here = key_cache[sequence].reshape(span, KVH, HD).astype(jnp.float32)
        value_here = value_cache[sequence].reshape(span, KVH, HD).astype(jnp.float32)
        scores = jnp.einsum('bgrd,cgd->grbc', query_blocks[slot_index].astype(jnp.float32), key_here) * (1.0 / math.sqrt(HD))
        scores = jnp.where(allowed[None, None], scores, -1e+30)
        largest = lax.optimization_barrier(jnp.max(scores, axis=-1, keepdims=True))
        weights = jnp.exp(scores - largest)
        probs = (weights / lax.optimization_barrier(jnp.sum(weights, axis=-1, keepdims=True))).astype(jnp.bfloat16)
        mixed = jnp.einsum('grbc,cgd->bgrd', probs.astype(jnp.float32), value_here)
        mixed = jnp.where((query_pos < length)[:, None, None, None], mixed, 0.0)
        return mixed.reshape(BLOCK, HQ * HD).astype(jnp.bfloat16)
    context = lax.map(attend, slot_ids).reshape(total, HQ * HD)
    return (context, key_cache, value_cache)
```

```python
import functools
import math

import jax
import jax.numpy as jnp
from jax import lax
from jax.experimental import pallas as pl
from jax.experimental.pallas import tpu as pltpu
from jax.sharding import PartitionSpec as P

HQ = 64
KVH = 8
HD = 128
BLOCK = 128
MAXB = 4


def rotate(field, positions):
    halfway = field.shape[-1] // 2
    indices = jnp.arange(halfway, dtype=jnp.float32)
    frequency = jnp.exp(-(2.0 * indices / field.shape[-1]) * math.log(500000.0))
    angles = positions[:, None] * frequency[None, :]
    cosines = jnp.cos(angles)[:, None, :]
    sines = jnp.sin(angles)[:, None, :]
    front = field[..., :halfway]
    back = field[..., halfway:]
    return jnp.concatenate(
        [front * cosines - back * sines, back * cosines + front * sines], axis=-1
    )


def shards(hidden, w_key, w_value, queries, lengths, seq_of_slot, pos_of_slot):
    replica = lax.axis_index("dp")
    token_rows = hidden.shape[0]
    local_slots = token_rows // BLOCK
    key_full, value_full = (
        lax.all_gather(w_key, "dp", axis=1, tiled=True),
        lax.all_gather(w_value, "dp", axis=1, tiled=True),
    )
    key_sum = jnp.dot(hidden, key_full, preferred_element_type=jnp.float32)
    value_sum = jnp.dot(hidden, value_full, preferred_element_type=jnp.float32)
    key_raw, value_raw = (
        lax.psum_scatter(key_sum, "mp", scatter_dimension=1, tiled=True),
        lax.psum_scatter(value_sum, "mp", scatter_dimension=1, tiled=True),
    )
    head_width = key_raw.shape[1]
    local_heads = head_width // HD
    my_seq = lax.dynamic_slice_in_dim(seq_of_slot, replica * local_slots, local_slots)
    my_pos = lax.dynamic_slice_in_dim(pos_of_slot, replica * local_slots, local_slots)
    offsets = jnp.arange(BLOCK, dtype=jnp.int32)
    query_pos = my_pos[:, None] * BLOCK + offsets[None, :]
    key_rows = rotate(
        key_raw.reshape(token_rows, local_heads, HD),
        query_pos.reshape(token_rows).astype(jnp.float32),
    )
    key_rows = key_rows.reshape(token_rows, head_width).astype(jnp.bfloat16)
    value_rows = value_raw.astype(jnp.bfloat16)
    payload = jnp.concatenate([key_rows, value_rows], axis=1).reshape(
        local_slots, BLOCK * 2 * head_width
    )
    blocks = jnp.arange(MAXB, dtype=jnp.int32)
    needed = (
        (seq_of_slot[None, None, :] == my_seq[:, None, None])
        & (pos_of_slot[None, None, :] == blocks[None, :, None])
        & (blocks[None, :, None] < my_pos[:, None, None])
    )
    owned = (seq_of_slot[None, :] == replica) & (pos_of_slot[None, :] == blocks[:, None])
    needed_pick = needed.astype(jnp.bfloat16)
    owned_pick = owned.astype(jnp.bfloat16)
    portion = lax.all_gather(payload, "dp", axis=0, tiled=True)
    earlier = jnp.einsum("smn,nx->smx", needed_pick, portion, preferred_element_type=jnp.float32)
    home_rows = jnp.dot(owned_pick, portion, preferred_element_type=jnp.float32)
    own_block = (blocks[None, :] == my_pos[:, None]).astype(jnp.float32)
    assembled = (earlier + own_block[:, :, None] * payload[:, None, :].astype(jnp.float32)).astype(
        jnp.bfloat16
    )
    span = MAXB * BLOCK
    assembled = assembled.reshape(local_slots, span, 2 * head_width)
    key_blocks = assembled[:, :, :head_width].reshape(local_slots, span, local_heads, HD)
    value_blocks = assembled[:, :, head_width:].reshape(local_slots, span, local_heads, HD)
    ratio = HQ // KVH
    query_blocks = queries.reshape(local_slots, BLOCK, local_heads, ratio, HD)
    scores = jnp.einsum(
        "sbgrd,scgd->sgrbc", query_blocks, key_blocks, preferred_element_type=jnp.float32
    ) * (1.0 / math.sqrt(HD))
    slot_lengths = lengths[my_seq]
    cached = jnp.arange(span, dtype=jnp.int32)
    allowed = (cached[None, None, :] <= query_pos[:, :, None]) & (
        cached[None, None, :] < slot_lengths[:, None, None]
    )
    scores = jnp.where(allowed[:, None, None], scores, -1e30)
    largest = jnp.max(scores, axis=-1, keepdims=True)
    weights = jnp.exp(scores - largest)
    probs = (weights / jnp.sum(weights, axis=-1, keepdims=True)).astype(jnp.bfloat16)
    mixed = jnp.einsum("sgrbc,scgd->sbgrd", probs, value_blocks, preferred_element_type=jnp.float32)
    valid = query_pos < slot_lengths[:, None]
    mixed = jnp.where(valid[:, :, None, None, None], mixed, 0.0)
    context = mixed.reshape(token_rows, local_heads * ratio * HD).astype(jnp.bfloat16)
    cache_rows = home_rows.reshape(span, 2 * head_width)
    own_length = lax.dynamic_slice_in_dim(lengths, replica, 1)[0]
    cache_rows = jnp.where((cached < own_length)[:, None], cache_rows, 0.0).astype(jnp.bfloat16)
    return (context, cache_rows[None, :, :head_width], cache_rows[None, :, head_width:])


MESH = pl.DeviceIdType.MESH
PIECES = 4
PAIR = 2
NEAR = (0, -1, 1)
UNITS = ((0, 2), (2, 6), (0, 4))


def when_all(conditions, action):
    live = [c for c in conditions if c is not None]
    if not live:
        action()
        return
    test = live[0]
    for c in live[1:]:
        test = jnp.logical_and(test, c)
    pl.when(test)(action)


def rebuild_kernel(
    depth,
    hidden_ref,
    wk_ref,
    wv_ref,
    q_ref,
    len_ref,
    seq_ref,
    pos_ref,
    ctx_out,
    key_out,
    value_out,
    hid,
    wt,
    acc,
    peer,
    xs,
    xr,
    kv0,
    kv1,
    sel,
    home_sel,
    arr0,
    arr1,
    home0,
    home1,
    qv,
    ctx0,
    ctx1,
    kc,
    vc,
    cos_t,
    sin_t,
    local_sem,
    send_sem,
    w_recv,
    h_recv,
    p_recv,
    x_recv,
    z_recv,
    u_recv,
):
    me = lax.axis_index("dp")
    core = lax.axis_index("mp")
    x = me % 2
    y = (me // 2) % 2
    z = me // 4
    mine = y * 2 + x
    rows = hidden_ref.shape[0]
    feats = hid.shape[2]
    wide = wk_ref.shape[0]
    kvs = (kv0, kv1)
    ctxs = (ctx0, ctx1)
    arrs = (arr0, arr1)
    homes = (home0, home1)
    slots = rows // BLOCK
    plane_slots = 4 * slots
    across = (z * 4 + y * 2 + (1 - x), core)
    along = (z * 4 + (1 - y) * 2 + x, core)
    diagonal = (z * 4 + (1 - y) * 2 + (1 - x), core)
    other = (me, 1 - core)
    targets = (across, along, diagonal)
    plane_ids = (y * 2 + 1 - x, (1 - y) * 2 + x, (1 - y) * 2 + 1 - x)
    my_feats = pl.ds(pl.multiple_of(x * feats, 128), feats)
    nbr_feats = pl.ds(pl.multiple_of((1 - x) * feats, 128), feats)
    sends = []

    def up():
        return z + 1 < depth

    def down():
        return z > 0

    def exists(dz):
        if dz == 0:
            return None
        return z + dz < depth if dz > 0 else z + dz >= 0

    def to_z(sign):
        return (me + 4 * sign, core)

    def remote(src, dst, sem, device):
        copy = pltpu.make_async_remote_copy(
            src_ref=src,
            dst_ref=dst,
            send_sem=send_sem.at[len(sends)],
            recv_sem=sem,
            device_id=device,
            device_id_type=MESH,
        )
        return copy

    def send(conditions, src, dst, sem, device):
        copy = remote(src, dst, sem, device)
        sends.append((conditions, copy))
        when_all(conditions, copy.start)

    def arrived(conditions, dst, sem):
        copy = pltpu.make_async_remote_copy(
            src_ref=dst,
            dst_ref=dst,
            send_sem=send_sem.at[0],
            recv_sem=sem,
            device_id=across,
            device_id_type=MESH,
        )
        when_all(conditions, copy.wait_recv)

    def w_piece(zc, kv, side):
        half = x if side == 0 else 1 - x
        return wt.at[zc, pl.ds(pl.multiple_of(kv * 2 * wide + half * wide, wide), wide)]

    def w_sem(zc, kv, side):
        return w_recv.at[zc * 4 + kv * 2 + side]

    half_q = qv.shape[2]
    order = (1 - core, core)
    local = []
    for i, (src, dst) in enumerate(
        [
            (hidden_ref.at[:, my_feats], hid.at[mine]),
            (wk_ref.at[:, my_feats], w_piece(z, 0, 0)),
            (wv_ref.at[:, my_feats], w_piece(z, 1, 0)),
        ]
        + [
            (q_ref.at[:, pl.ds(pl.multiple_of(order[j] * half_q, 128), half_q)], qv.at[j])
            for j in range(2)
        ]
    ):
        copy = pltpu.make_async_copy(src, dst, local_sem.at[i])
        copy.start()
        local.append(copy)

    barrier = pltpu.get_barrier_semaphore()

    def greet(device):
        pl.semaphore_signal(barrier, inc=1, device_id=device, device_id_type=MESH)

    for device in (across, along, diagonal, other):
        greet(device)
    pl.when(down())(lambda: greet(to_z(-1)))
    pl.when(up())(lambda: greet(to_z(1)))
    inner = jnp.logical_and(down(), up())
    pl.when(inner)(lambda: pl.semaphore_wait(barrier, 6))
    pl.when(jnp.logical_not(inner))(lambda: pl.semaphore_wait(barrier, 5))

    weights = (wk_ref, wv_ref)
    for kv in range(2):
        send([up()], weights[kv].at[:, my_feats], w_piece(z, kv, 0), w_sem(z, kv, 0), to_z(1))
        send([down()], weights[kv].at[:, my_feats], w_piece(z, kv, 0), w_sem(z, kv, 0), to_z(-1))
        give = wt.at[z, pl.ds(pl.multiple_of(kv * 2 * wide + x * wide, wide), wide)]
        send([], weights[kv].at[:, nbr_feats], give, w_sem(z, kv, 1), across)
    step = rows // PIECES
    for p in range(PIECES):
        part = pl.ds(p * step, step)
        send([], hidden_ref.at[part, nbr_feats], hid.at[mine, part], h_recv.at[mine * PIECES + p], across)
        send([], hidden_ref.at[part, my_feats], hid.at[mine, part], h_recv.at[mine * PIECES + p], along)

    total_slots = base = seq_ref.shape[0]
    replicas = [z * 4 + i for i in plane_ids] + [me]
    wanted = []
    for r in replicas:
        wanted += [seq_ref[r * slots + s] for s in range(slots)] + [r]

    def scan(n, found):
        s, m = seq_ref[n], pos_ref[n]
        weight = jnp.where(m == 0, 1, jnp.where(m == 1, base, jnp.where(m == 2, base**2, base**3)))
        coded = n * weight
        return tuple(f + jnp.where(s == w, coded, 0) for f, w in zip(found, wanted))

    found = (0,) * len(wanted)
    for n in range(total_slots):
        found = scan(n, found)
    picks = []
    for t in range(4):
        codes = found[3 * t : 3 * t + 3]
        early = [(codes[s] // base**m) % base for s in range(slots) for m in range(MAXB - 1)]
        home = [(codes[slots] // base**m) % base for m in range(MAXB)]
        picks.append((early, home))

    def tables():
        lane = lax.broadcasted_iota(jnp.int32, (BLOCK, HD), 1)
        indices = (lane % (HD // 2)).astype(jnp.float32)
        frequency = jnp.exp(-(2.0 * indices / HD) * math.log(500000.0))
        row = lax.broadcasted_iota(jnp.int32, (BLOCK, HD), 0)
        for i in range(plane_slots):
            start = pos_ref[z * plane_slots + i] * BLOCK
            angles = (start + row).astype(jnp.float32) * frequency
            cos_t[pl.ds(i * BLOCK, BLOCK)] = jnp.cos(angles)
            sines = jnp.sin(angles)
            sin_t[pl.ds(i * BLOCK, BLOCK)] = jnp.where(lane < HD // 2, -sines, sines)

    pl.when(x == 0)(tables)

    def w_arrive(dz, side):
        zc = z + dz
        here = exists(dz)
        for kv in range(2):
            piece = w_piece(zc, kv, side)
            sem = w_sem(zc, kv, side)
            arrived([here], piece, sem)
            if dz == 0:
                send([up()], piece, piece, sem, to_z(1))
                send([down()], piece, piece, sem, to_z(-1))
            elif abs(dz) < depth - 1:
                sign = 1 if dz < 0 else -1
                send([here, up() if sign > 0 else down()], piece, piece, sem, to_z(sign))

    def h_forward(p):
        part = pl.ds(p * step, step)
        src = plane_ids[0]
        block = hid.at[src, part]
        arrived([], block, h_recv.at[src * PIECES + p])
        send([], block, block, h_recv.at[src * PIECES + p], along)

    w_arrive(0, 1)
    w_arrive(-1, 0)
    w_arrive(1, 0)
    h_forward(0)
    h_forward(1)
    w_arrive(-1, 1)
    w_arrive(1, 1)
    h_forward(2)
    h_forward(3)
    w_arrive(-2, 0)
    w_arrive(2, 0)
    for copy in local:
        copy.wait()
    for p in range(PIECES):
        for src in plane_ids[1:]:
            arrived([], hid.at[src, pl.ds(p * step, step)], h_recv.at[src * PIECES + p])

    def owner(dz):
        return (z + dz) // 2

    def multiply(dz):
        zc = z + dz

        def run():
            for i in range(4):
                block = lax.dot_general(
                    hid[i], wt[zc], (((1,), (1,)), ((), ())), preferred_element_type=jnp.float32
                )
                part = pl.ds(i * rows, rows)
                acc[zc, 0, part] = block[:, :HD]
                acc[zc, 1, part] = block[:, HD:]

        when_all([exists(dz)], run)
        send(
            [exists(dz), owner(dz) != core],
            acc.at[zc],
            peer.at[zc % 2],
            p_recv.at[zc % 2],
            other,
        )

    def reduce(dz):
        zc = z + dz
        k = zc % 2
        mine_here = [exists(dz), owner(dz) == core]
        arrived(mine_here, peer.at[k], p_recv.at[k])

        def body():
            xs[k] = (acc[zc, 1 - x] + peer[k, 1 - x]).astype(jnp.bfloat16)

        when_all(mine_here, body)
        send(mine_here, xs.at[k], xr.at[k], x_recv.at[k], across)

    def finish(dz):
        zc = z + dz
        k = zc % 2
        outer = 1 - ((zc + 1) // 2) % 2
        arrived([exists(dz), owner(dz) == core], xr.at[k], x_recv.at[k])
        for j in range(2):
            kv = kvs[j]
            mine_here = [exists(dz), owner(dz) == core, outer == j]

            def body(kv=kv, j=j):
                for i in range(plane_slots):
                    part = pl.ds(i * BLOCK, BLOCK)
                    total = acc[zc, x, part] + peer[k, x, part] + xr[k, part].astype(jnp.float32)

                    def turn(total=total, part=part, i=i):
                        turned = total * cos_t[part] + pltpu.roll(total, HD // 2, 1) * sin_t[part]
                        kv[z * plane_slots + i] = turned.astype(jnp.bfloat16)

                    def keep(total=total, i=i):
                        kv[z * plane_slots + i] = total.astype(jnp.bfloat16)

                    pl.when(x == 0)(turn)
                    pl.when(x != 0)(keep)

            when_all(mine_here, body)
            block = kv.at[pl.ds(z * plane_slots, plane_slots)]
            send(mine_here + [up()], block, block, z_recv.at[j * depth + z], to_z(1))
            send(mine_here + [down()], block, block, z_recv.at[j * depth + z], to_z(-1))

    def kv_arrive(j, dz):
        here = exists(dz)
        block = kvs[j].at[pl.ds((z + dz) * plane_slots, plane_slots)]
        sem = z_recv.at[j * depth + z + dz]
        sign = 1 if dz < 0 else -1
        onward = up() if sign > 0 else down()
        arrived([here, onward], block, sem)
        if abs(dz) < depth - 1:
            send([here, onward], block, block, sem, to_z(sign))

    def kv_last(j, dz):
        sign = 1 if dz < 0 else -1
        onward = up() if sign > 0 else down()
        block = kvs[j].at[pl.ds((z + dz) * plane_slots, plane_slots)]
        arrived([exists(dz), jnp.logical_not(onward)], block, z_recv.at[j * depth + z + dz])

    def unit_sem(j, t, kind):
        return u_recv.at[(j * 3 + t) * 3 + kind]

    def give_own(j):
        for t in range(3):
            src = kvs[j].at[pl.ds(z * plane_slots + plane_ids[t] * slots, slots)]
            send([], src, arrs[j].at[mine, pl.ds(0, slots)], unit_sem(j, t, 0), targets[t])
        arrs[j][mine, pl.ds(0, slots)] = kvs[j][pl.ds(me * slots, slots)]

    def landing(j, src, kind):
        return (homes if kind == 2 else arrs)[j].at[src, pl.ds(*UNITS[kind])]

    def give_picked(j):
        kv = kvs[j]
        for kind, staged in ((1, sel), (2, home_sel)):
            for t in (2, 0, 1):
                for u in range(UNITS[kind][1]):
                    staged[j, t, u] = kv[picks[t][kind - 1][u]]
                send([], staged.at[j, t], landing(j, mine, kind), unit_sem(j, t, kind), targets[t])
        for u in range(UNITS[1][1]):
            arrs[j][mine, UNITS[1][0] + u] = kv[picks[3][0][u]]
        for u in range(UNITS[2][1]):
            homes[j][mine, u] = kv[picks[3][1][u]]

    def units_arrive(j, kind):
        for t in range(3):
            arrived([], landing(j, plane_ids[t], kind), unit_sem(j, t, kind))

    ratio = half_q // (2 * HD)
    head_span = ratio * HD
    outs = {}

    def copy_out(name, src, dst, sem):
        if name in outs:
            outs[name].wait()
        outs[name] = pltpu.make_async_copy(src, dst, local_sem.at[sem])
        outs[name].start()

    def attend(j):
        units_arrive(j, 0)
        units_arrive(j, 1)
        earlier = MAXB - 1

        def body(i, _):
            s = i // 2
            h = i % 2
            q_pos = pos_ref[me * slots + s]
            length = len_ref[seq_ref[me * slots + s]]
            row = lax.broadcasted_iota(jnp.int32, (BLOCK, BLOCK), 0)
            col = lax.broadcasted_iota(jnp.int32, (BLOCK, BLOCK), 1)
            start = q_pos * BLOCK
            parts = [jnp.where((col <= row) & (start + col < length), 0.0, -1e30)]
            for m in range(earlier):
                parts.append(jnp.full((BLOCK, BLOCK), jnp.where(m < q_pos, 0.0, -1e30), jnp.float32))
            bias = jnp.concatenate(parts, axis=1)
            bias = jnp.concatenate([bias] * PAIR, axis=0)
            valid = (start + row) < length
            span = MAXB * BLOCK
            pieces = []
            for kv in range(2):
                own = arrs[j][2 * h + kv, s]
                rest = arrs[j][2 * h + kv, pl.ds(slots + s * earlier, earlier)]
                pieces.append(
                    jnp.concatenate([own, rest.reshape(earlier * BLOCK, HD)], axis=0)
                )
            keys, values = pieces
            part = pl.ds(pl.multiple_of(s * BLOCK, BLOCK), BLOCK)

            def columns(r):
                return pl.ds(pl.multiple_of(h * head_span + r * HD, HD), HD)

            for r in range(0, ratio, PAIR):
                q = jnp.concatenate([qv[j, part, columns(r + i)] for i in range(PAIR)], axis=0)
                scores = lax.dot_general(
                    q, keys, (((1,), (1,)), ((), ())), preferred_element_type=jnp.float32
                )
                scores = scores + bias
                largest = jnp.max(scores, axis=1, keepdims=True)
                exps = jnp.exp2((scores - largest) * (math.log2(math.e) / math.sqrt(HD)))
                scale = 1.0 / jnp.sum(exps, axis=1, keepdims=True)
                mixed = jnp.dot(exps.astype(jnp.bfloat16), values, preferred_element_type=jnp.float32)
                mixed = mixed * scale
                for i in range(PAIR):
                    piece = jnp.where(valid, mixed[i * BLOCK : (i + 1) * BLOCK], 0.0)
                    ctxs[j][part, columns(r + i)] = piece.astype(jnp.bfloat16)
            return 0

        lax.fori_loop(0, 2 * slots, body, 0)
        target = ctx_out.at[:, pl.ds(pl.multiple_of(order[j] * half_q, 128), half_q)]
        copy_out("context", ctxs[j], target, 5 + j)

    def caches(j):
        units_arrive(j, 2)
        length = len_ref[me]
        for m in range(MAXB):
            place = m * BLOCK + lax.broadcasted_iota(jnp.int32, (BLOCK, HD), 0)
            for h in range(2):
                for kv, out in ((0, kc), (1, vc)):
                    block = homes[j][2 * h + kv, m]
                    out[j, pl.ds(m * BLOCK, BLOCK), pl.ds(h * HD, HD)] = jnp.where(
                        place < length, block, jnp.zeros_like(block)
                    )
        column = pl.ds(pl.multiple_of(order[j] * 2 * HD, 128), 2 * HD)
        copy_out("keys", kc.at[j], key_out.at[0, :, column], 7 + 2 * j)
        copy_out("values", vc.at[j], value_out.at[0, :, column], 8 + 2 * j)

    for dz in NEAR:
        multiply(dz)
    w_arrive(-2, 1)
    w_arrive(2, 1)
    for dz in NEAR:
        reduce(dz)
    multiply(-2)
    multiply(2)
    for dz in NEAR:
        finish(dz)
    for dz in (-2, 2):
        reduce(dz)
    for dz in (-2, 2):
        finish(dz)
    give_own(0)
    for dz in (-1, 1, -2, 2):
        kv_arrive(0, dz)
    w_arrive(-3, 0)
    w_arrive(3, 0)
    w_arrive(-3, 1)
    w_arrive(3, 1)
    for dz in (-3, 3):
        multiply(dz)
    for dz in (-3, 3):
        reduce(dz)
    for dz in (-3, 3):
        finish(dz)
    give_own(1)
    for dz in (-1, 1, -2, 2, -3, 3):
        kv_last(0, dz)
    give_picked(0)
    for dz in (-1, 1, -2, 2):
        kv_arrive(1, dz)
    attend(0)
    caches(0)
    for dz in (-1, 1, -2, 2, -3, 3):
        kv_last(1, dz)
    give_picked(1)
    attend(1)
    caches(1)
    for copy in outs.values():
        copy.wait()
    for conditions, copy in sends:
        when_all(conditions, copy.wait_send)


def fast_shards(hidden, w_key, w_value, queries, lengths, seq_of_slot, pos_of_slot):
    depth = lax.axis_size("dp") // 4
    rows, features = hidden.shape
    wide = w_key.shape[1]
    slots = rows // BLOCK
    local_heads = wide * 4 * depth // HD // 2
    half = features // 2
    total = seq_of_slot.shape[0]
    plane = 4 * rows
    dma = pltpu.SemaphoreType.DMA
    anywhere = pl.BlockSpec(memory_space=pl.ANY)
    smem = pl.BlockSpec(memory_space=pltpu.SMEM)
    cache = jax.ShapeDtypeStruct((1, MAXB * BLOCK, local_heads * HD), jnp.bfloat16)
    bf16, f32 = jnp.bfloat16, jnp.float32
    half_q = queries.shape[1] // 2
    return pl.pallas_call(
        functools.partial(rebuild_kernel, depth),
        out_shape=(jax.ShapeDtypeStruct(queries.shape, bf16), cache, cache),
        in_specs=[anywhere] * 4 + [smem] * 3,
        out_specs=(anywhere,) * 3,
        scratch_shapes=[
            pltpu.VMEM((4, rows, half), bf16),
            pltpu.VMEM((depth, 4 * wide, half), bf16),
            pltpu.VMEM((depth, 2, plane, HD), f32),
            pltpu.VMEM((2, 2, plane, HD), f32),
            pltpu.VMEM((2, plane, HD), bf16),
            pltpu.VMEM((2, plane, HD), bf16),
            pltpu.VMEM((total, BLOCK, HD), bf16),
            pltpu.VMEM((total, BLOCK, HD), bf16),
            pltpu.VMEM((2, 3, 6, BLOCK, HD), bf16),
            pltpu.VMEM((2, 3, 4, BLOCK, HD), bf16),
            pltpu.VMEM((4, 8, BLOCK, HD), bf16),
            pltpu.VMEM((4, 8, BLOCK, HD), bf16),
            pltpu.VMEM((4, 4, BLOCK, HD), bf16),
            pltpu.VMEM((4, 4, BLOCK, HD), bf16),
            pltpu.VMEM((2, rows, half_q), bf16),
            pltpu.VMEM((rows, half_q), bf16),
            pltpu.VMEM((rows, half_q), bf16),
            pltpu.VMEM((2, MAXB * BLOCK, 2 * HD), bf16),
            pltpu.VMEM((2, MAXB * BLOCK, 2 * HD), bf16),
            pltpu.VMEM((plane, HD), f32),
            pltpu.VMEM((plane, HD), f32),
            dma((11,)),
            dma((128,)),
            dma((4 * depth,)),
            dma((4 * PIECES,)),
            dma((2,)),
            dma((2,)),
            dma((2 * depth,)),
            dma((18,)),
        ],
        compiler_params=pltpu.CompilerParams(
            collective_id=0, has_side_effects=True, vmem_limit_bytes=60 * 2**20
        ),
    )(hidden, w_key.T, w_value.T, queries, lengths, seq_of_slot, pos_of_slot)


def suits(mesh):
    replicas, halves = mesh.shape["dp"], mesh.shape["mp"]
    return halves == 2 and replicas % 8 == 0 and KVH * HD == replicas * (HD // 2)


def solution(mesh):
    in_specs = (P("dp", "mp"), P("mp", "dp"), P("mp", "dp"), P("dp", "mp"), P(), P(), P())
    out_specs = (P("dp", "mp"), P("dp", None, "mp"), P("dp", None, "mp"))
    return jax.shard_map(fast_shards if suits(mesh) else shards, mesh=mesh, in_specs=in_specs, out_specs=out_specs, check_vma=False)
```

```python
import functools
import math

import jax
import jax.numpy as jnp
from jax import lax
from jax.experimental import pallas as pl
from jax.experimental.pallas import tpu as pltpu
from jax.sharding import PartitionSpec as P

HQ = 64
KVH = 8
HD = 128
BLOCK = 128
MAXB = 4


def rotate(field, positions):
    halfway = field.shape[-1] // 2
    indices = jnp.arange(halfway, dtype=jnp.float32)
    frequency = jnp.exp(-(2.0 * indices / field.shape[-1]) * math.log(500000.0))
    angles = positions[:, None] * frequency[None, :]
    cosines = jnp.cos(angles)[:, None, :]
    sines = jnp.sin(angles)[:, None, :]
    front = field[..., :halfway]
    back = field[..., halfway:]
    return jnp.concatenate(
        [front * cosines - back * sines, back * cosines + front * sines], axis=-1
    )


def shards(hidden, w_key, w_value, queries, lengths, seq_of_slot, pos_of_slot):
    replica = lax.axis_index("dp")
    token_rows = hidden.shape[0]
    local_slots = token_rows // BLOCK
    key_full, value_full = (
        lax.all_gather(w_key, "dp", axis=1, tiled=True),
        lax.all_gather(w_value, "dp", axis=1, tiled=True),
    )
    key_sum = jnp.dot(hidden, key_full, preferred_element_type=jnp.float32)
    value_sum = jnp.dot(hidden, value_full, preferred_element_type=jnp.float32)
    key_raw, value_raw = (
        lax.psum_scatter(key_sum, "mp", scatter_dimension=1, tiled=True),
        lax.psum_scatter(value_sum, "mp", scatter_dimension=1, tiled=True),
    )
    head_width = key_raw.shape[1]
    local_heads = head_width // HD
    my_seq = lax.dynamic_slice_in_dim(seq_of_slot, replica * local_slots, local_slots)
    my_pos = lax.dynamic_slice_in_dim(pos_of_slot, replica * local_slots, local_slots)
    offsets = jnp.arange(BLOCK, dtype=jnp.int32)
    query_pos = my_pos[:, None] * BLOCK + offsets[None, :]
    key_rows = rotate(
        key_raw.reshape(token_rows, local_heads, HD),
        query_pos.reshape(token_rows).astype(jnp.float32),
    )
    key_rows = key_rows.reshape(token_rows, head_width).astype(jnp.bfloat16)
    value_rows = value_raw.astype(jnp.bfloat16)
    payload = jnp.concatenate([key_rows, value_rows], axis=1).reshape(
        local_slots, BLOCK * 2 * head_width
    )
    blocks = jnp.arange(MAXB, dtype=jnp.int32)
    needed = (
        (seq_of_slot[None, None, :] == my_seq[:, None, None])
        & (pos_of_slot[None, None, :] == blocks[None, :, None])
        & (blocks[None, :, None] < my_pos[:, None, None])
    )
    owned = (seq_of_slot[None, :] == replica) & (pos_of_slot[None, :] == blocks[:, None])
    needed_pick = needed.astype(jnp.bfloat16)
    owned_pick = owned.astype(jnp.bfloat16)
    portion = lax.all_gather(payload, "dp", axis=0, tiled=True)
    earlier = jnp.einsum("smn,nx->smx", needed_pick, portion, preferred_element_type=jnp.float32)
    home_rows = jnp.dot(owned_pick, portion, preferred_element_type=jnp.float32)
    own_block = (blocks[None, :] == my_pos[:, None]).astype(jnp.float32)
    assembled = (earlier + own_block[:, :, None] * payload[:, None, :].astype(jnp.float32)).astype(
        jnp.bfloat16
    )
    span = MAXB * BLOCK
    assembled = assembled.reshape(local_slots, span, 2 * head_width)
    key_blocks = assembled[:, :, :head_width].reshape(local_slots, span, local_heads, HD)
    value_blocks = assembled[:, :, head_width:].reshape(local_slots, span, local_heads, HD)
    ratio = HQ // KVH
    query_blocks = queries.reshape(local_slots, BLOCK, local_heads, ratio, HD)
    scores = jnp.einsum(
        "sbgrd,scgd->sgrbc", query_blocks, key_blocks, preferred_element_type=jnp.float32
    ) * (1.0 / math.sqrt(HD))
    slot_lengths = lengths[my_seq]
    cached = jnp.arange(span, dtype=jnp.int32)
    allowed = (cached[None, None, :] <= query_pos[:, :, None]) & (
        cached[None, None, :] < slot_lengths[:, None, None]
    )
    scores = jnp.where(allowed[:, None, None], scores, -1e30)
    largest = jnp.max(scores, axis=-1, keepdims=True)
    weights = jnp.exp(scores - largest)
    probs = (weights / jnp.sum(weights, axis=-1, keepdims=True)).astype(jnp.bfloat16)
    mixed = jnp.einsum("sgrbc,scgd->sbgrd", probs, value_blocks, preferred_element_type=jnp.float32)
    valid = query_pos < slot_lengths[:, None]
    mixed = jnp.where(valid[:, :, None, None, None], mixed, 0.0)
    context = mixed.reshape(token_rows, local_heads * ratio * HD).astype(jnp.bfloat16)
    cache_rows = home_rows.reshape(span, 2 * head_width)
    own_length = lax.dynamic_slice_in_dim(lengths, replica, 1)[0]
    cache_rows = jnp.where((cached < own_length)[:, None], cache_rows, 0.0).astype(jnp.bfloat16)
    return (context, cache_rows[None, :, :head_width], cache_rows[None, :, head_width:])


MESH = pl.DeviceIdType.MESH
PIECES = 4
PAIR = 2
NEAR = (0, -1, 1)
UNITS = ((0, 2), (2, 6), (0, 4))


def when_all(conditions, action):
    live = [c for c in conditions if c is not None]
    if not live:
        action()
        return
    test = live[0]
    for c in live[1:]:
        test = jnp.logical_and(test, c)
    pl.when(test)(action)


def rebuild_kernel(
    depth,
    hidden_ref,
    wk_ref,
    wv_ref,
    q_ref,
    len_ref,
    seq_ref,
    pos_ref,
    ctx_out,
    key_out,
    value_out,
    hid,
    wt,
    acc,
    peer,
    xs,
    xr,
    kv0,
    kv1,
    sel,
    home_sel,
    arr0,
    arr1,
    home0,
    home1,
    qv,
    cos_t,
    sin_t,
    local_sem,
    send_sem,
    w_recv,
    h_recv,
    p_recv,
    x_recv,
    z_recv,
    u_recv,
):
    me = lax.axis_index("dp")
    core = lax.axis_index("mp")
    x = me % 2
    y = (me // 2) % 2
    z = me // 4
    mine = y * 2 + x
    rows = hidden_ref.shape[0]
    feats = hid.shape[2]
    wide = wk_ref.shape[0]
    kvs = (kv0, kv1)
    arrs = (arr0, arr1)
    homes = (home0, home1)
    slots = rows // BLOCK
    plane_slots = 4 * slots
    across = (z * 4 + y * 2 + (1 - x), core)
    along = (z * 4 + (1 - y) * 2 + x, core)
    diagonal = (z * 4 + (1 - y) * 2 + (1 - x), core)
    other = (me, 1 - core)
    targets = (across, along, diagonal)
    plane_ids = (y * 2 + 1 - x, (1 - y) * 2 + x, (1 - y) * 2 + 1 - x)
    my_feats = pl.ds(pl.multiple_of(x * feats, 128), feats)
    nbr_feats = pl.ds(pl.multiple_of((1 - x) * feats, 128), feats)
    sends = []

    def up():
        return z + 1 < depth

    def down():
        return z > 0

    def exists(dz):
        if dz == 0:
            return None
        return z + dz < depth if dz > 0 else z + dz >= 0

    def to_z(sign):
        return (me + 4 * sign, core)

    def remote(src, dst, sem, device):
        copy = pltpu.make_async_remote_copy(
            src_ref=src,
            dst_ref=dst,
            send_sem=send_sem.at[len(sends)],
            recv_sem=sem,
            device_id=device,
            device_id_type=MESH,
        )
        return copy

    def send(conditions, src, dst, sem, device):
        copy = remote(src, dst, sem, device)
        sends.append((conditions, copy))
        when_all(conditions, copy.start)

    def arrived(conditions, dst, sem):
        copy = pltpu.make_async_remote_copy(
            src_ref=dst,
            dst_ref=dst,
            send_sem=send_sem.at[0],
            recv_sem=sem,
            device_id=across,
            device_id_type=MESH,
        )
        when_all(conditions, copy.wait_recv)

    def w_piece(zc, kv, side):
        half = x if side == 0 else 1 - x
        return wt.at[zc, pl.ds(pl.multiple_of(kv * 2 * wide + half * wide, wide), wide)]

    def w_sem(zc, kv, side):
        return w_recv.at[zc * 4 + kv * 2 + side]

    half_q = qv.shape[2]
    order = (1 - core, core)
    local = []
    for i, (src, dst) in enumerate(
        [
            (hidden_ref.at[:, my_feats], hid.at[mine]),
            (wk_ref.at[:, my_feats], w_piece(z, 0, 0)),
            (wv_ref.at[:, my_feats], w_piece(z, 1, 0)),
        ]
        + [
            (q_ref.at[:, pl.ds(pl.multiple_of(order[j] * half_q, 128), half_q)], qv.at[j])
            for j in range(2)
        ]
    ):
        copy = pltpu.make_async_copy(src, dst, local_sem.at[i])
        copy.start()
        local.append(copy)

    barrier = pltpu.get_barrier_semaphore()

    def greet(device):
        pl.semaphore_signal(barrier, inc=1, device_id=device, device_id_type=MESH)

    for device in (across, along, diagonal, other):
        greet(device)
    pl.when(down())(lambda: greet(to_z(-1)))
    pl.when(up())(lambda: greet(to_z(1)))
    inner = jnp.logical_and(down(), up())
    pl.when(inner)(lambda: pl.semaphore_wait(barrier, 6))
    pl.when(jnp.logical_not(inner))(lambda: pl.semaphore_wait(barrier, 5))

    weights = (wk_ref, wv_ref)
    for kv in range(2):
        send([up()], weights[kv].at[:, my_feats], w_piece(z, kv, 0), w_sem(z, kv, 0), to_z(1))
        send([down()], weights[kv].at[:, my_feats], w_piece(z, kv, 0), w_sem(z, kv, 0), to_z(-1))
        give = wt.at[z, pl.ds(pl.multiple_of(kv * 2 * wide + x * wide, wide), wide)]
        send([], weights[kv].at[:, nbr_feats], give, w_sem(z, kv, 1), across)
    step = rows // PIECES
    for p in range(PIECES):
        part = pl.ds(p * step, step)
        send([], hidden_ref.at[part, nbr_feats], hid.at[mine, part], h_recv.at[mine * PIECES + p], across)
        send([], hidden_ref.at[part, my_feats], hid.at[mine, part], h_recv.at[mine * PIECES + p], along)

    total_slots = base = seq_ref.shape[0]
    replicas = [z * 4 + i for i in plane_ids] + [me]
    wanted = []
    for r in replicas:
        wanted += [seq_ref[r * slots + s] for s in range(slots)] + [r]

    def scan(n, found):
        s, m = seq_ref[n], pos_ref[n]
        weight = jnp.where(m == 0, 1, jnp.where(m == 1, base, jnp.where(m == 2, base**2, base**3)))
        coded = n * weight
        return tuple(f + jnp.where(s == w, coded, 0) for f, w in zip(found, wanted))

    found = (0,) * len(wanted)
    for n in range(total_slots):
        found = scan(n, found)
    picks = []
    for t in range(4):
        codes = found[3 * t : 3 * t + 3]
        early = [(codes[s] // base**m) % base for s in range(slots) for m in range(MAXB - 1)]
        home = [(codes[slots] // base**m) % base for m in range(MAXB)]
        picks.append((early, home))

    def tables():
        lane = lax.broadcasted_iota(jnp.int32, (BLOCK, HD), 1)
        indices = (lane % (HD // 2)).astype(jnp.float32)
        frequency = jnp.exp(-(2.0 * indices / HD) * math.log(500000.0))
        row = lax.broadcasted_iota(jnp.int32, (BLOCK, HD), 0)
        for i in range(plane_slots):
            start = pos_ref[z * plane_slots + i] * BLOCK
            angles = (start + row).astype(jnp.float32) * frequency
            cos_t[pl.ds(i * BLOCK, BLOCK)] = jnp.cos(angles)
            sines = jnp.sin(angles)
            sin_t[pl.ds(i * BLOCK, BLOCK)] = jnp.where(lane < HD // 2, -sines, sines)

    pl.when(x == 0)(tables)

    def w_arrive(dz, side):
        zc = z + dz
        here = exists(dz)
        for kv in range(2):
            piece = w_piece(zc, kv, side)
            sem = w_sem(zc, kv, side)
            arrived([here], piece, sem)
            if dz == 0:
                send([up()], piece, piece, sem, to_z(1))
                send([down()], piece, piece, sem, to_z(-1))
            elif abs(dz) < depth - 1:
                sign = 1 if dz < 0 else -1
                send([here, up() if sign > 0 else down()], piece, piece, sem, to_z(sign))

    def h_forward(p):
        part = pl.ds(p * step, step)
        src = plane_ids[0]
        block = hid.at[src, part]
        arrived([], block, h_recv.at[src * PIECES + p])
        send([], block, block, h_recv.at[src * PIECES + p], along)

    w_arrive(0, 1)
    w_arrive(-1, 0)
    w_arrive(1, 0)
    h_forward(0)
    h_forward(1)
    w_arrive(-1, 1)
    w_arrive(1, 1)
    h_forward(2)
    h_forward(3)
    w_arrive(-2, 0)
    w_arrive(2, 0)
    for copy in local:
        copy.wait()
    for p in range(PIECES):
        for src in plane_ids[1:]:
            arrived([], hid.at[src, pl.ds(p * step, step)], h_recv.at[src * PIECES + p])

    def owner(dz):
        return (z + dz) // 2

    def multiply(dz):
        zc = z + dz

        def run():
            for i in range(4):
                block = lax.dot_general(
                    hid[i], wt[zc], (((1,), (1,)), ((), ())), preferred_element_type=jnp.float32
                )
                part = pl.ds(i * rows, rows)
                acc[zc, 0, part] = block[:, :HD]
                acc[zc, 1, part] = block[:, HD:]

        when_all([exists(dz)], run)
        send(
            [exists(dz), owner(dz) != core],
            acc.at[zc],
            peer.at[zc % 2],
            p_recv.at[zc % 2],
            other,
        )

    def reduce(dz):
        zc = z + dz
        k = zc % 2
        mine_here = [exists(dz), owner(dz) == core]
        arrived(mine_here, peer.at[k], p_recv.at[k])

        def body():
            xs[k] = (acc[zc, 1 - x] + peer[k, 1 - x]).astype(jnp.bfloat16)

        when_all(mine_here, body)
        send(mine_here, xs.at[k], xr.at[k], x_recv.at[k], across)

    def finish(dz):
        zc = z + dz
        k = zc % 2
        outer = 1 - ((zc + 1) // 2) % 2
        arrived([exists(dz), owner(dz) == core], xr.at[k], x_recv.at[k])
        for j in range(2):
            kv = kvs[j]
            mine_here = [exists(dz), owner(dz) == core, outer == j]

            def body(kv=kv, j=j):
                for i in range(plane_slots):
                    part = pl.ds(i * BLOCK, BLOCK)
                    total = acc[zc, x, part] + peer[k, x, part] + xr[k, part].astype(jnp.float32)

                    def turn(total=total, part=part, i=i):
                        turned = total * cos_t[part] + pltpu.roll(total, HD // 2, 1) * sin_t[part]
                        kv[z * plane_slots + i] = turned.astype(jnp.bfloat16)

                    def keep(total=total, i=i):
                        kv[z * plane_slots + i] = total.astype(jnp.bfloat16)

                    pl.when(x == 0)(turn)
                    pl.when(x != 0)(keep)

            when_all(mine_here, body)
            block = kv.at[pl.ds(z * plane_slots, plane_slots)]
            send(mine_here + [up()], block, block, z_recv.at[j * depth + z], to_z(1))
            send(mine_here + [down()], block, block, z_recv.at[j * depth + z], to_z(-1))

    def kv_arrive(j, dz):
        here = exists(dz)
        block = kvs[j].at[pl.ds((z + dz) * plane_slots, plane_slots)]
        sem = z_recv.at[j * depth + z + dz]
        sign = 1 if dz < 0 else -1
        onward = up() if sign > 0 else down()
        arrived([here, onward], block, sem)
        if abs(dz) < depth - 1:
            send([here, onward], block, block, sem, to_z(sign))

    def kv_last(j, dz):
        sign = 1 if dz < 0 else -1
        onward = up() if sign > 0 else down()
        block = kvs[j].at[pl.ds((z + dz) * plane_slots, plane_slots)]
        arrived([exists(dz), jnp.logical_not(onward)], block, z_recv.at[j * depth + z + dz])

    def unit_sem(j, t, kind):
        return u_recv.at[(j * 3 + t) * 3 + kind]

    def give_own(j):
        for t in range(3):
            src = kvs[j].at[pl.ds(z * plane_slots + plane_ids[t] * slots, slots)]
            send([], src, arrs[j].at[mine, pl.ds(0, slots)], unit_sem(j, t, 0), targets[t])
        arrs[j][mine, pl.ds(0, slots)] = kvs[j][pl.ds(me * slots, slots)]

    def landing(j, src, kind):
        return (homes if kind == 2 else arrs)[j].at[src, pl.ds(*UNITS[kind])]

    def give_picked(j):
        kv = kvs[j]
        for kind, staged in ((1, sel), (2, home_sel)):
            for t in range(3):
                for u in range(UNITS[kind][1]):
                    staged[j, t, u] = kv[picks[t][kind - 1][u]]
                send([], staged.at[j, t], landing(j, mine, kind), unit_sem(j, t, kind), targets[t])
        for u in range(UNITS[1][1]):
            arrs[j][mine, UNITS[1][0] + u] = kv[picks[3][0][u]]
        for u in range(UNITS[2][1]):
            homes[j][mine, u] = kv[picks[3][1][u]]

    def units_arrive(j, kind):
        for t in range(3):
            arrived([], landing(j, plane_ids[t], kind), unit_sem(j, t, kind))

    ratio = half_q // (2 * HD)
    head_span = ratio * HD
    def attend(j):
        for part, head in ((0, y), (1, 1 - y)):
            for t in range(3)[part : 2 * part + 1]:
                for kind in range(2):
                    arrived([], landing(j, plane_ids[t], kind), unit_sem(j, t, kind))
            lax.fori_loop(0, slots, functools.partial(attend_head, j, head), 0)

    def attend_head(j, h, s, _):
        earlier = MAXB - 1
        q_pos = pos_ref[me * slots + s]
        length = len_ref[seq_ref[me * slots + s]]
        row = lax.broadcasted_iota(jnp.int32, (BLOCK, BLOCK), 0)
        col = lax.broadcasted_iota(jnp.int32, (BLOCK, BLOCK), 1)
        start = q_pos * BLOCK
        parts = [jnp.where((col <= row) & (start + col < length), 0.0, -1e30)]
        for m in range(earlier):
            parts.append(jnp.full((BLOCK, BLOCK), jnp.where(m < q_pos, 0.0, -1e30), jnp.float32))
        bias = jnp.concatenate(parts, axis=1)
        bias = jnp.concatenate([bias] * PAIR, axis=0)
        valid = (start + row) < length
        pieces = []
        for kv in range(2):
            own = arrs[j][2 * h + kv, s]
            rest = arrs[j][2 * h + kv, pl.ds(slots + s * earlier, earlier)]
            pieces.append(jnp.concatenate([own, rest.reshape(earlier * BLOCK, HD)], axis=0))
        keys, values = pieces
        part = pl.ds(pl.multiple_of(s * BLOCK, BLOCK), BLOCK)
        for r in range(0, ratio, PAIR):
            q = jnp.concatenate(
                [
                    qv[j, part, pl.ds(pl.multiple_of(h * head_span + (r + i) * HD, HD), HD)]
                    for i in range(PAIR)
                ],
                axis=0,
            )
            scores = lax.dot_general(
                q, keys, (((1,), (1,)), ((), ())), preferred_element_type=jnp.float32
            )
            scores = scores + bias
            largest = jnp.max(scores, axis=1, keepdims=True)
            exps = jnp.exp2((scores - largest) * (math.log2(math.e) / math.sqrt(HD)))
            scale = 1.0 / jnp.sum(exps, axis=1, keepdims=True)
            mixed = jnp.dot(exps.astype(jnp.bfloat16), values, preferred_element_type=jnp.float32)
            mixed = mixed * scale
            for i in range(PAIR):
                piece = jnp.where(valid, mixed[i * BLOCK : (i + 1) * BLOCK], 0.0)
                place = order[j] * half_q + h * head_span + (r + i) * HD
                ctx_out[part, pl.ds(pl.multiple_of(place, HD), HD)] = piece.astype(jnp.bfloat16)
        return 0

    def caches(j):
        units_arrive(j, 2)
        length = len_ref[me]
        for m in range(MAXB):
            place = m * BLOCK + lax.broadcasted_iota(jnp.int32, (BLOCK, HD), 0)
            for h in range(2):
                column = pl.ds(pl.multiple_of((order[j] * 2 + h) * HD, HD), HD)
                for kv, out in ((0, key_out), (1, value_out)):
                    block = homes[j][2 * h + kv, m]
                    out[0, pl.ds(m * BLOCK, BLOCK), column] = jnp.where(
                        place < length, block, jnp.zeros_like(block)
                    )

    for dz in NEAR:
        multiply(dz)
    w_arrive(-2, 1)
    w_arrive(2, 1)
    for dz in NEAR:
        reduce(dz)
    multiply(-2)
    multiply(2)
    for dz in NEAR:
        finish(dz)
    for dz in (-2, 2):
        reduce(dz)
    for dz in (-2, 2):
        finish(dz)
    give_own(0)
    for dz in (-1, 1, -2, 2):
        kv_arrive(0, dz)
    w_arrive(-3, 0)
    w_arrive(3, 0)
    w_arrive(-3, 1)
    w_arrive(3, 1)
    for dz in (-3, 3):
        multiply(dz)
    for dz in (-3, 3):
        reduce(dz)
    for dz in (-3, 3):
        finish(dz)
    give_own(1)
    for dz in (-1, 1, -2, 2, -3, 3):
        kv_last(0, dz)
    give_picked(0)
    for dz in (-1, 1, -2, 2):
        kv_arrive(1, dz)
    attend(0)
    caches(0)
    for dz in (-1, 1, -2, 2, -3, 3):
        kv_last(1, dz)
    give_picked(1)
    attend(1)
    caches(1)
    for conditions, copy in sends:
        when_all(conditions, copy.wait_send)


def fast_shards(hidden, w_key, w_value, queries, lengths, seq_of_slot, pos_of_slot):
    depth = lax.axis_size("dp") // 4
    rows, features = hidden.shape
    wide = w_key.shape[1]
    slots = rows // BLOCK
    local_heads = wide * 4 * depth // HD // 2
    half = features // 2
    total = seq_of_slot.shape[0]
    plane = 4 * rows
    dma = pltpu.SemaphoreType.DMA
    anywhere = pl.BlockSpec(memory_space=pltpu.HBM)
    vmem = pl.BlockSpec(memory_space=pltpu.VMEM)
    smem = pl.BlockSpec(memory_space=pltpu.SMEM)
    bf16, f32 = jnp.bfloat16, jnp.float32
    cache = pltpu.VMEM((1, MAXB * BLOCK, local_heads * HD), bf16)
    half_q = queries.shape[1] // 2
    return pl.pallas_call(
        functools.partial(rebuild_kernel, depth),
        out_shape=(pltpu.VMEM(queries.shape, bf16), cache, cache),
        in_specs=[anywhere] * 4 + [smem] * 3,
        out_specs=(vmem,) * 3,
        scratch_shapes=[
            pltpu.VMEM((4, rows, half), bf16),
            pltpu.VMEM((depth, 4 * wide, half), bf16),
            pltpu.VMEM((depth, 2, plane, HD), f32),
            pltpu.VMEM((2, 2, plane, HD), f32),
            pltpu.VMEM((2, plane, HD), bf16),
            pltpu.VMEM((2, plane, HD), bf16),
            pltpu.VMEM((total, BLOCK, HD), bf16),
            pltpu.VMEM((total, BLOCK, HD), bf16),
            pltpu.VMEM((2, 3, 6, BLOCK, HD), bf16),
            pltpu.VMEM((2, 3, 4, BLOCK, HD), bf16),
            pltpu.VMEM((4, 8, BLOCK, HD), bf16),
            pltpu.VMEM((4, 8, BLOCK, HD), bf16),
            pltpu.VMEM((4, 4, BLOCK, HD), bf16),
            pltpu.VMEM((4, 4, BLOCK, HD), bf16),
            pltpu.VMEM((2, rows, half_q), bf16),
            pltpu.VMEM((plane, HD), f32),
            pltpu.VMEM((plane, HD), f32),
            dma((5,)),
            dma((128,)),
            dma((4 * depth,)),
            dma((4 * PIECES,)),
            dma((2,)),
            dma((2,)),
            dma((2 * depth,)),
            dma((18,)),
        ],
        compiler_params=pltpu.CompilerParams(
            collective_id=0, has_side_effects=True, vmem_limit_bytes=62300 * 2**10
        ),
    )(hidden, w_key.T, w_value.T, queries, lengths, seq_of_slot, pos_of_slot)


def suits(mesh):
    replicas, halves = mesh.shape["dp"], mesh.shape["mp"]
    return halves == 2 and replicas % 8 == 0 and KVH * HD == replicas * (HD // 2)


def solution(mesh):
    in_specs = (P("dp", "mp"), P("mp", "dp"), P("mp", "dp"), P("dp", "mp"), P(), P(), P())
    out_specs = (P("dp", "mp"), P("dp", None, "mp"), P("dp", None, "mp"))
    return jax.shard_map(fast_shards if suits(mesh) else shards, mesh=mesh, in_specs=in_specs, out_specs=out_specs, check_vma=False)
```

```python
import functools
import math

import jax
import jax.numpy as jnp
from jax import lax
from jax.experimental import pallas as pl
from jax.experimental.pallas import tpu as pltpu
from jax.sharding import PartitionSpec as P

HQ = 64
KVH = 8
HD = 128
BLOCK = 128
MAXB = 4


def rotate(field, positions):
    halfway = field.shape[-1] // 2
    indices = jnp.arange(halfway, dtype=jnp.float32)
    frequency = jnp.exp(-(2.0 * indices / field.shape[-1]) * math.log(500000.0))
    angles = positions[:, None] * frequency[None, :]
    cosines = jnp.cos(angles)[:, None, :]
    sines = jnp.sin(angles)[:, None, :]
    front = field[..., :halfway]
    back = field[..., halfway:]
    return jnp.concatenate(
        [front * cosines - back * sines, back * cosines + front * sines], axis=-1
    )


def shards(hidden, w_key, w_value, queries, lengths, seq_of_slot, pos_of_slot):
    replica = lax.axis_index("dp")
    token_rows = hidden.shape[0]
    local_slots = token_rows // BLOCK
    key_full, value_full = (
        lax.all_gather(w_key, "dp", axis=1, tiled=True),
        lax.all_gather(w_value, "dp", axis=1, tiled=True),
    )
    key_sum = jnp.dot(hidden, key_full, preferred_element_type=jnp.float32)
    value_sum = jnp.dot(hidden, value_full, preferred_element_type=jnp.float32)
    key_raw, value_raw = (
        lax.psum_scatter(key_sum, "mp", scatter_dimension=1, tiled=True),
        lax.psum_scatter(value_sum, "mp", scatter_dimension=1, tiled=True),
    )
    head_width = key_raw.shape[1]
    local_heads = head_width // HD
    my_seq = lax.dynamic_slice_in_dim(seq_of_slot, replica * local_slots, local_slots)
    my_pos = lax.dynamic_slice_in_dim(pos_of_slot, replica * local_slots, local_slots)
    offsets = jnp.arange(BLOCK, dtype=jnp.int32)
    query_pos = my_pos[:, None] * BLOCK + offsets[None, :]
    key_rows = rotate(
        key_raw.reshape(token_rows, local_heads, HD),
        query_pos.reshape(token_rows).astype(jnp.float32),
    )
    key_rows = key_rows.reshape(token_rows, head_width).astype(jnp.bfloat16)
    value_rows = value_raw.astype(jnp.bfloat16)
    payload = jnp.concatenate([key_rows, value_rows], axis=1).reshape(
        local_slots, BLOCK * 2 * head_width
    )
    blocks = jnp.arange(MAXB, dtype=jnp.int32)
    needed = (
        (seq_of_slot[None, None, :] == my_seq[:, None, None])
        & (pos_of_slot[None, None, :] == blocks[None, :, None])
        & (blocks[None, :, None] < my_pos[:, None, None])
    )
    owned = (seq_of_slot[None, :] == replica) & (pos_of_slot[None, :] == blocks[:, None])
    needed_pick = needed.astype(jnp.bfloat16)
    owned_pick = owned.astype(jnp.bfloat16)
    portion = lax.all_gather(payload, "dp", axis=0, tiled=True)
    earlier = jnp.einsum("smn,nx->smx", needed_pick, portion, preferred_element_type=jnp.float32)
    home_rows = jnp.dot(owned_pick, portion, preferred_element_type=jnp.float32)
    own_block = (blocks[None, :] == my_pos[:, None]).astype(jnp.float32)
    assembled = (earlier + own_block[:, :, None] * payload[:, None, :].astype(jnp.float32)).astype(
        jnp.bfloat16
    )
    span = MAXB * BLOCK
    assembled = assembled.reshape(local_slots, span, 2 * head_width)
    key_blocks = assembled[:, :, :head_width].reshape(local_slots, span, local_heads, HD)
    value_blocks = assembled[:, :, head_width:].reshape(local_slots, span, local_heads, HD)
    ratio = HQ // KVH
    query_blocks = queries.reshape(local_slots, BLOCK, local_heads, ratio, HD)
    scores = jnp.einsum(
        "sbgrd,scgd->sgrbc", query_blocks, key_blocks, preferred_element_type=jnp.float32
    ) * (1.0 / math.sqrt(HD))
    slot_lengths = lengths[my_seq]
    cached = jnp.arange(span, dtype=jnp.int32)
    allowed = (cached[None, None, :] <= query_pos[:, :, None]) & (
        cached[None, None, :] < slot_lengths[:, None, None]
    )
    scores = jnp.where(allowed[:, None, None], scores, -1e30)
    largest = jnp.max(scores, axis=-1, keepdims=True)
    weights = jnp.exp(scores - largest)
    probs = (weights / jnp.sum(weights, axis=-1, keepdims=True)).astype(jnp.bfloat16)
    mixed = jnp.einsum("sgrbc,scgd->sbgrd", probs, value_blocks, preferred_element_type=jnp.float32)
    valid = query_pos < slot_lengths[:, None]
    mixed = jnp.where(valid[:, :, None, None, None], mixed, 0.0)
    context = mixed.reshape(token_rows, local_heads * ratio * HD).astype(jnp.bfloat16)
    cache_rows = home_rows.reshape(span, 2 * head_width)
    own_length = lax.dynamic_slice_in_dim(lengths, replica, 1)[0]
    cache_rows = jnp.where((cached < own_length)[:, None], cache_rows, 0.0).astype(jnp.bfloat16)
    return (context, cache_rows[None, :, :head_width], cache_rows[None, :, head_width:])


MESH = pl.DeviceIdType.MESH
PIECES = 4
PAIR = 2
NEAR = (0, -1, 1)
UNITS = ((0, 2), (2, 6), (0, 4))


def when_all(conditions, action):
    live = [c for c in conditions if c is not None]
    if not live:
        action()
        return
    test = live[0]
    for c in live[1:]:
        test = jnp.logical_and(test, c)
    pl.when(test)(action)


def rebuild_kernel(
    depth,
    hidden_ref,
    wk_ref,
    wv_ref,
    q_ref,
    len_ref,
    seq_ref,
    pos_ref,
    ctx_out,
    key_out,
    value_out,
    hid,
    wt,
    acc,
    peer,
    xs,
    xr,
    kv0,
    kv1,
    kv2,
    kv3,
    sel,
    home_sel,
    arr0,
    arr1,
    home0,
    home1,
    qv,
    cos_t,
    sin_t,
    local_sem,
    send_sem,
    w_recv,
    h_recv,
    p_recv,
    x_recv,
    z_recv,
    u_recv,
):
    me = lax.axis_index("dp")
    core = lax.axis_index("mp")
    x = me % 2
    y = (me // 2) % 2
    z = me // 4
    mine = y * 2 + x
    rows = hidden_ref.shape[0]
    feats = hid.shape[2]
    wide = wk_ref.shape[0]
    kvs = (kv0, kv1, kv2, kv3)
    half = BLOCK // 2
    arrs = (arr0, arr1)
    homes = (home0, home1)
    slots = rows // BLOCK
    plane_slots = 4 * slots
    across = (z * 4 + y * 2 + (1 - x), core)
    along = (z * 4 + (1 - y) * 2 + x, core)
    diagonal = (z * 4 + (1 - y) * 2 + (1 - x), core)
    other = (me, 1 - core)
    targets = (across, along, diagonal)
    plane_ids = (y * 2 + 1 - x, (1 - y) * 2 + x, (1 - y) * 2 + 1 - x)
    my_feats = pl.ds(pl.multiple_of(x * feats, 128), feats)
    nbr_feats = pl.ds(pl.multiple_of((1 - x) * feats, 128), feats)
    sends = []

    def up():
        return z + 1 < depth

    def down():
        return z > 0

    def exists(dz):
        if dz == 0:
            return None
        return z + dz < depth if dz > 0 else z + dz >= 0

    def to_z(sign):
        return (me + 4 * sign, core)

    def remote(src, dst, sem, device):
        copy = pltpu.make_async_remote_copy(
            src_ref=src,
            dst_ref=dst,
            send_sem=send_sem.at[len(sends)],
            recv_sem=sem,
            device_id=device,
            device_id_type=MESH,
        )
        return copy

    def send(conditions, src, dst, sem, device):
        copy = remote(src, dst, sem, device)
        sends.append((conditions, copy))
        assert len(sends) <= send_sem.shape[0]
        when_all(conditions, copy.start)

    def arrived(conditions, dst, sem):
        copy = pltpu.make_async_remote_copy(
            src_ref=dst,
            dst_ref=dst,
            send_sem=send_sem.at[0],
            recv_sem=sem,
            device_id=across,
            device_id_type=MESH,
        )
        when_all(conditions, copy.wait_recv)

    def w_piece(zc, kv, side):
        half = x if side == 0 else 1 - x
        return wt.at[zc, pl.ds(pl.multiple_of(kv * 2 * wide + half * wide, wide), wide)]

    def w_sem(zc, kv, side):
        return w_recv.at[zc * 4 + kv * 2 + side]

    half_q = qv.shape[2]
    order = (1 - core, core)
    local = []
    for i, (src, dst) in enumerate(
        [
            (hidden_ref.at[:, my_feats], hid.at[mine]),
            (wk_ref.at[:, my_feats], w_piece(z, 0, 0)),
            (wv_ref.at[:, my_feats], w_piece(z, 1, 0)),
        ]
        + [
            (q_ref.at[:, pl.ds(pl.multiple_of(order[j] * half_q, 128), half_q)], qv.at[j])
            for j in range(2)
        ]
    ):
        copy = pltpu.make_async_copy(src, dst, local_sem.at[i])
        copy.start()
        local.append(copy)

    barrier = pltpu.get_barrier_semaphore()

    def greet(device):
        pl.semaphore_signal(barrier, inc=1, device_id=device, device_id_type=MESH)

    for device in (across, along, diagonal, other):
        greet(device)
    pl.when(down())(lambda: greet(to_z(-1)))
    pl.when(up())(lambda: greet(to_z(1)))
    inner = jnp.logical_and(down(), up())
    pl.when(inner)(lambda: pl.semaphore_wait(barrier, 6))
    pl.when(jnp.logical_not(inner))(lambda: pl.semaphore_wait(barrier, 5))

    weights = (wk_ref, wv_ref)
    for kv in range(2):
        send([up()], weights[kv].at[:, my_feats], w_piece(z, kv, 0), w_sem(z, kv, 0), to_z(1))
        send([down()], weights[kv].at[:, my_feats], w_piece(z, kv, 0), w_sem(z, kv, 0), to_z(-1))
        give = wt.at[z, pl.ds(pl.multiple_of(kv * 2 * wide + x * wide, wide), wide)]
        send([], weights[kv].at[:, nbr_feats], give, w_sem(z, kv, 1), across)
    step = rows // PIECES
    for p in range(PIECES):
        part = pl.ds(p * step, step)
        send([], hidden_ref.at[part, nbr_feats], hid.at[mine, part], h_recv.at[mine * PIECES + p], across)
        send([], hidden_ref.at[part, my_feats], hid.at[mine, part], h_recv.at[mine * PIECES + p], along)

    total_slots = base = seq_ref.shape[0]
    replicas = [z * 4 + i for i in plane_ids] + [me]
    wanted = []
    for r in replicas:
        wanted += [seq_ref[r * slots + s] for s in range(slots)] + [r]

    def scan(n, found):
        s, m = seq_ref[n], pos_ref[n]
        weight = jnp.where(m == 0, 1, jnp.where(m == 1, base, jnp.where(m == 2, base**2, base**3)))
        coded = n * weight
        return tuple(f + jnp.where(s == w, coded, 0) for f, w in zip(found, wanted))

    found = (0,) * len(wanted)
    for n in range(total_slots):
        found = scan(n, found)
    picks = []
    for t in range(4):
        codes = found[3 * t : 3 * t + 3]
        early = [(codes[s] // base**m) % base for s in range(slots) for m in range(MAXB - 1)]
        home = [(codes[slots] // base**m) % base for m in range(MAXB)]
        picks.append((early, home))

    def tables():
        lane = lax.broadcasted_iota(jnp.int32, (BLOCK, HD), 1)
        indices = (lane % (HD // 2)).astype(jnp.float32)
        frequency = jnp.exp(-(2.0 * indices / HD) * math.log(500000.0))
        row = lax.broadcasted_iota(jnp.int32, (BLOCK, HD), 0)
        for i in range(plane_slots):
            start = pos_ref[z * plane_slots + i] * BLOCK
            angles = (start + row).astype(jnp.float32) * frequency
            cos_t[pl.ds(i * BLOCK, BLOCK)] = jnp.cos(angles)
            sines = jnp.sin(angles)
            sin_t[pl.ds(i * BLOCK, BLOCK)] = jnp.where(lane < HD // 2, -sines, sines)

    pl.when(x == 0)(tables)

    def w_arrive(dz, side):
        zc = z + dz
        here = exists(dz)
        for kv in range(2):
            piece = w_piece(zc, kv, side)
            sem = w_sem(zc, kv, side)
            arrived([here], piece, sem)
            if dz == 0:
                send([up()], piece, piece, sem, to_z(1))
                send([down()], piece, piece, sem, to_z(-1))
            elif abs(dz) < depth - 1:
                sign = 1 if dz < 0 else -1
                send([here, up() if sign > 0 else down()], piece, piece, sem, to_z(sign))

    def h_forward(p):
        part = pl.ds(p * step, step)
        src = plane_ids[0]
        block = hid.at[src, part]
        arrived([], block, h_recv.at[src * PIECES + p])
        send([], block, block, h_recv.at[src * PIECES + p], along)

    w_arrive(0, 1)
    w_arrive(-1, 0)
    w_arrive(1, 0)
    h_forward(0)
    h_forward(1)
    w_arrive(-1, 1)
    w_arrive(1, 1)
    h_forward(2)
    h_forward(3)
    w_arrive(-2, 0)
    w_arrive(2, 0)
    for copy in local:
        copy.wait()
    for p in range(PIECES):
        for src in plane_ids[1:]:
            arrived([], hid.at[src, pl.ds(p * step, step)], h_recv.at[src * PIECES + p])

    def owner(dz):
        return (z + dz) // 2

    def multiply(dz):
        zc = z + dz

        def run():
            for i in range(4):
                block = lax.dot_general(
                    hid[i], wt[zc], (((1,), (1,)), ((), ())), preferred_element_type=jnp.float32
                )
                part = pl.ds(i * rows, rows)
                acc[zc, 0, part] = block[:, :HD]
                acc[zc, 1, part] = block[:, HD:]

        when_all([exists(dz)], run)
        send(
            [exists(dz), owner(dz) != core],
            acc.at[zc],
            peer.at[zc % 2],
            p_recv.at[zc % 2],
            other,
        )

    def reduce(dz):
        zc = z + dz
        k = zc % 2
        mine_here = [exists(dz), owner(dz) == core]
        arrived(mine_here, peer.at[k], p_recv.at[k])

        def body():
            xs[k] = (acc[zc, 1 - x] + peer[k, 1 - x]).astype(jnp.bfloat16)

        when_all(mine_here, body)
        send(mine_here, xs.at[k], xr.at[k], x_recv.at[k], across)

    def finish(dz):
        zc = z + dz
        k = zc % 2
        outer = 1 - ((zc + 1) // 2) % 2
        arrived([exists(dz), owner(dz) == core], xr.at[k], x_recv.at[k])
        for j in range(2):

            def body(j=j):
                def store(i, block):
                    for p in range(2):
                        kvs[2 * j + p][z * plane_slots + i] = block[p * half : (p + 1) * half].astype(
                            jnp.bfloat16
                        )

                for i in range(plane_slots):
                    part = pl.ds(i * BLOCK, BLOCK)
                    total = acc[zc, x, part] + peer[k, x, part] + xr[k, part].astype(jnp.float32)

                    def turn(total=total, part=part, i=i):
                        store(i, total * cos_t[part] + pltpu.roll(total, HD // 2, 1) * sin_t[part])

                    pl.when(x == 0)(turn)
                    pl.when(x != 0)(functools.partial(store, i, total))

            when_all([exists(dz), owner(dz) == core, outer == j], body)

    def kv_part(p, plane):
        return kvs[p].at[pl.ds(plane * plane_slots, plane_slots)], z_recv.at[p * depth + plane]

    def own_sends(p, conditions):
        block, sem = kv_part(p, z)
        send(conditions + [up()], block, block, sem, to_z(1))
        send(conditions + [down()], block, block, sem, to_z(-1))

    def relay(p, dz, condition):
        block, sem = kv_part(p, z + dz)
        sign = 1 if dz < 0 else -1
        conditions = [condition, exists(dz), up() if sign > 0 else down()]
        arrived(conditions, block, sem)
        send(conditions, block, block, sem, to_z(sign))

    def relays(p):
        low = z * 2 < depth
        high = jnp.logical_not(low)
        for near, dz in ((1, 1), (-1, 1), (1, 2)):
            relay(p, near * dz, low)
            relay(p, -near * dz, high)

    def last(p):
        for dz in range(1, depth):
            for sign in (1, -1):
                block, sem = kv_part(p, z - sign * dz)
                onward = up() if sign > 0 else down()
                arrived([exists(-sign * dz), jnp.logical_not(onward)], block, sem)

    def unit_sem(p, t, kind):
        return u_recv.at[(p * 3 + t) * 3 + kind]

    def part_rows(p):
        return pl.ds(p % 2 * half, half)

    def landing(p, src, kind):
        return (homes if kind == 2 else arrs)[p // 2].at[src, pl.ds(*UNITS[kind]), part_rows(p)]

    def give_own(p):
        for t in range(3):
            src = kvs[p].at[pl.ds(z * plane_slots + plane_ids[t] * slots, slots)]
            send([], src, landing(p, mine, 0), unit_sem(p, t, 0), targets[t])
        arrs[p // 2][mine, pl.ds(0, slots), part_rows(p)] = kvs[p][pl.ds(me * slots, slots)]

    def give_picked(p):
        kv, j, part = kvs[p], p // 2, part_rows(p)
        for kind, staged in ((1, sel), (2, home_sel)):
            for t in range(3):
                for u in range(UNITS[kind][1]):
                    staged[j, t, u, part] = kv[picks[t][kind - 1][u]]
                send([], staged.at[j, t, :, part], landing(p, mine, kind), unit_sem(p, t, kind), targets[t])
        for u in range(UNITS[1][1]):
            arrs[j][mine, UNITS[1][0] + u, part] = kv[picks[3][0][u]]
        for u in range(UNITS[2][1]):
            homes[j][mine, u, part] = kv[picks[3][1][u]]

    def units_arrive(j, sources, kinds):
        for p in (2 * j, 2 * j + 1):
            for t in sources:
                for kind in kinds:
                    arrived([], landing(p, plane_ids[t], kind), unit_sem(p, t, kind))

    ratio = half_q // (2 * HD)
    head_span = ratio * HD
    def attend(j, part):
        units_arrive(j, (1, 2) if part else (0,), (0, 1))
        head = 1 - y if part else y
        lax.fori_loop(0, slots, functools.partial(attend_head, j, head), 0)

    def attend_head(j, h, s, _):
        earlier = MAXB - 1
        q_pos = pos_ref[me * slots + s]
        length = len_ref[seq_ref[me * slots + s]]
        row = lax.broadcasted_iota(jnp.int32, (BLOCK, BLOCK), 0)
        col = lax.broadcasted_iota(jnp.int32, (BLOCK, BLOCK), 1)
        start = q_pos * BLOCK
        parts = [jnp.where((col <= row) & (start + col < length), 0.0, -1e30)]
        for m in range(earlier):
            parts.append(jnp.full((BLOCK, BLOCK), jnp.where(m < q_pos, 0.0, -1e30), jnp.float32))
        bias = jnp.concatenate(parts, axis=1)
        bias = jnp.concatenate([bias] * PAIR, axis=0)
        valid = (start + row) < length
        pieces = []
        for kv in range(2):
            own = arrs[j][2 * h + kv, s]
            rest = arrs[j][2 * h + kv, pl.ds(slots + s * earlier, earlier)]
            pieces.append(jnp.concatenate([own, rest.reshape(earlier * BLOCK, HD)], axis=0))
        keys, values = pieces
        part = pl.ds(pl.multiple_of(s * BLOCK, BLOCK), BLOCK)
        for r in range(0, ratio, PAIR):
            q = jnp.concatenate(
                [
                    qv[j, part, pl.ds(pl.multiple_of(h * head_span + (r + i) * HD, HD), HD)]
                    for i in range(PAIR)
                ],
                axis=0,
            )
            scores = lax.dot_general(
                q, keys, (((1,), (1,)), ((), ())), preferred_element_type=jnp.float32
            )
            scores = scores + bias
            largest = jnp.max(scores, axis=1, keepdims=True)
            exps = jnp.exp2((scores - largest) * (math.log2(math.e) / math.sqrt(HD)))
            scale = 1.0 / jnp.sum(exps, axis=1, keepdims=True)
            mixed = jnp.dot(exps.astype(jnp.bfloat16), values, preferred_element_type=jnp.float32)
            mixed = mixed * scale
            for i in range(PAIR):
                piece = jnp.where(valid, mixed[i * BLOCK : (i + 1) * BLOCK], 0.0)
                place = order[j] * half_q + h * head_span + (r + i) * HD
                ctx_out[part, pl.ds(pl.multiple_of(place, HD), HD)] = piece.astype(jnp.bfloat16)
        return 0

    def caches(j):
        units_arrive(j, range(3), (2,))
        length = len_ref[me]
        for m in range(MAXB):
            place = m * BLOCK + lax.broadcasted_iota(jnp.int32, (BLOCK, HD), 0)
            for h in range(2):
                column = pl.ds(pl.multiple_of((order[j] * 2 + h) * HD, HD), HD)
                for kv, out in ((0, key_out), (1, value_out)):
                    block = homes[j][2 * h + kv, m]
                    out[0, pl.ds(m * BLOCK, BLOCK), column] = jnp.where(
                        place < length, block, jnp.zeros_like(block)
                    )

    for dz in NEAR:
        multiply(dz)
    w_arrive(-2, 1)
    w_arrive(2, 1)
    for dz in NEAR:
        reduce(dz)
    multiply(-2)
    multiply(2)
    for dz in NEAR:
        finish(dz)
    for dz in (-2, 2):
        reduce(dz)
    for dz in (-2, 2):
        finish(dz)
    edge = jnp.logical_not(inner)
    own_sends(0, [])
    give_own(0)
    relays(0)
    own_sends(1, [])
    give_own(1)
    relays(1)
    w_arrive(-3, 0)
    w_arrive(3, 0)
    w_arrive(-3, 1)
    w_arrive(3, 1)
    for dz in (-3, 3):
        multiply(dz)
    for dz in (-3, 3):
        reduce(dz)
    for dz in (-3, 3):
        finish(dz)
    for p in (2, 3):
        own_sends(p, [edge])
        give_own(p)
    for p in (0, 1):
        last(p)
        give_picked(p)
    for p in (2, 3):
        own_sends(p, [inner])
        relays(p)
    attend(0, 0)
    last(2)
    give_picked(2)
    attend(0, 1)
    caches(0)
    last(3)
    give_picked(3)
    attend(1, 0)
    attend(1, 1)
    caches(1)
    for conditions, copy in sends:
        when_all(conditions, copy.wait_send)


def fast_shards(hidden, w_key, w_value, queries, lengths, seq_of_slot, pos_of_slot):
    depth = lax.axis_size("dp") // 4
    rows, features = hidden.shape
    wide = w_key.shape[1]
    slots = rows // BLOCK
    local_heads = wide * 4 * depth // HD // 2
    half = features // 2
    total = seq_of_slot.shape[0]
    plane = 4 * rows
    dma = pltpu.SemaphoreType.DMA
    anywhere = pl.BlockSpec(memory_space=pltpu.HBM)
    vmem = pl.BlockSpec(memory_space=pltpu.VMEM)
    smem = pl.BlockSpec(memory_space=pltpu.SMEM)
    bf16, f32 = jnp.bfloat16, jnp.float32
    cache = pltpu.VMEM((1, MAXB * BLOCK, local_heads * HD), bf16)
    half_q = queries.shape[1] // 2
    return pl.pallas_call(
        functools.partial(rebuild_kernel, depth),
        out_shape=(pltpu.VMEM(queries.shape, bf16), cache, cache),
        in_specs=[anywhere] * 4 + [smem] * 3,
        out_specs=(vmem,) * 3,
        scratch_shapes=[
            pltpu.VMEM((4, rows, half), bf16),
            pltpu.VMEM((depth, 4 * wide, half), bf16),
            pltpu.VMEM((depth, 2, plane, HD), f32),
            pltpu.VMEM((2, 2, plane, HD), f32),
            pltpu.VMEM((2, plane, HD), bf16),
            pltpu.VMEM((2, plane, HD), bf16),
        ]
        + [pltpu.VMEM((total, BLOCK // 2, HD), bf16)] * 4
        + [
            pltpu.VMEM((2, 3, 6, BLOCK, HD), bf16),
            pltpu.VMEM((2, 3, 4, BLOCK, HD), bf16),
            pltpu.VMEM((4, 8, BLOCK, HD), bf16),
            pltpu.VMEM((4, 8, BLOCK, HD), bf16),
            pltpu.VMEM((4, 4, BLOCK, HD), bf16),
            pltpu.VMEM((4, 4, BLOCK, HD), bf16),
            pltpu.VMEM((2, rows, half_q), bf16),
            pltpu.VMEM((plane, HD), f32),
            pltpu.VMEM((plane, HD), f32),
            dma((5,)),
            dma((192,)),
            dma((4 * depth,)),
            dma((4 * PIECES,)),
            dma((2,)),
            dma((2,)),
            dma((4 * depth,)),
            dma((36,)),
        ],
        compiler_params=pltpu.CompilerParams(
            collective_id=0, has_side_effects=True, vmem_limit_bytes=62300 * 2**10
        ),
    )(hidden, w_key.T, w_value.T, queries, lengths, seq_of_slot, pos_of_slot)


def suits(mesh):
    replicas, halves = mesh.shape["dp"], mesh.shape["mp"]
    return halves == 2 and replicas % 8 == 0 and KVH * HD == replicas * (HD // 2)


def solution(mesh):
    in_specs = (P("dp", "mp"), P("mp", "dp"), P("mp", "dp"), P("dp", "mp"), P(), P(), P())
    out_specs = (P("dp", "mp"), P("dp", None, "mp"), P("dp", None, "mp"))
    return jax.shard_map(fast_shards if suits(mesh) else shards, mesh=mesh, in_specs=in_specs, out_specs=out_specs, check_vma=False)
```

```python
import functools
import math

import jax
import jax.numpy as jnp
from jax import lax
from jax.experimental import pallas as pl
from jax.experimental.pallas import tpu as pltpu
from jax.sharding import PartitionSpec as P

HQ = 64
KVH = 8
HD = 128
BLOCK = 128
MAXB = 4


def rotate(field, positions):
    halfway = field.shape[-1] // 2
    indices = jnp.arange(halfway, dtype=jnp.float32)
    frequency = jnp.exp(-(2.0 * indices / field.shape[-1]) * math.log(500000.0))
    angles = positions[:, None] * frequency[None, :]
    cosines = jnp.cos(angles)[:, None, :]
    sines = jnp.sin(angles)[:, None, :]
    front = field[..., :halfway]
    back = field[..., halfway:]
    return jnp.concatenate(
        [front * cosines - back * sines, back * cosines + front * sines], axis=-1
    )


def shards(hidden, w_key, w_value, queries, lengths, seq_of_slot, pos_of_slot):
    replica = lax.axis_index("dp")
    token_rows = hidden.shape[0]
    local_slots = token_rows // BLOCK
    key_full, value_full = (
        lax.all_gather(w_key, "dp", axis=1, tiled=True),
        lax.all_gather(w_value, "dp", axis=1, tiled=True),
    )
    key_sum = jnp.dot(hidden, key_full, preferred_element_type=jnp.float32)
    value_sum = jnp.dot(hidden, value_full, preferred_element_type=jnp.float32)
    key_raw, value_raw = (
        lax.psum_scatter(key_sum, "mp", scatter_dimension=1, tiled=True),
        lax.psum_scatter(value_sum, "mp", scatter_dimension=1, tiled=True),
    )
    head_width = key_raw.shape[1]
    local_heads = head_width // HD
    my_seq = lax.dynamic_slice_in_dim(seq_of_slot, replica * local_slots, local_slots)
    my_pos = lax.dynamic_slice_in_dim(pos_of_slot, replica * local_slots, local_slots)
    offsets = jnp.arange(BLOCK, dtype=jnp.int32)
    query_pos = my_pos[:, None] * BLOCK + offsets[None, :]
    key_rows = rotate(
        key_raw.reshape(token_rows, local_heads, HD),
        query_pos.reshape(token_rows).astype(jnp.float32),
    )
    key_rows = key_rows.reshape(token_rows, head_width).astype(jnp.bfloat16)
    value_rows = value_raw.astype(jnp.bfloat16)
    payload = jnp.concatenate([key_rows, value_rows], axis=1).reshape(
        local_slots, BLOCK * 2 * head_width
    )
    blocks = jnp.arange(MAXB, dtype=jnp.int32)
    needed = (
        (seq_of_slot[None, None, :] == my_seq[:, None, None])
        & (pos_of_slot[None, None, :] == blocks[None, :, None])
        & (blocks[None, :, None] < my_pos[:, None, None])
    )
    owned = (seq_of_slot[None, :] == replica) & (pos_of_slot[None, :] == blocks[:, None])
    needed_pick = needed.astype(jnp.bfloat16)
    owned_pick = owned.astype(jnp.bfloat16)
    portion = lax.all_gather(payload, "dp", axis=0, tiled=True)
    earlier = jnp.einsum("smn,nx->smx", needed_pick, portion, preferred_element_type=jnp.float32)
    home_rows = jnp.dot(owned_pick, portion, preferred_element_type=jnp.float32)
    own_block = (blocks[None, :] == my_pos[:, None]).astype(jnp.float32)
    assembled = (earlier + own_block[:, :, None] * payload[:, None, :].astype(jnp.float32)).astype(
        jnp.bfloat16
    )
    span = MAXB * BLOCK
    assembled = assembled.reshape(local_slots, span, 2 * head_width)
    key_blocks = assembled[:, :, :head_width].reshape(local_slots, span, local_heads, HD)
    value_blocks = assembled[:, :, head_width:].reshape(local_slots, span, local_heads, HD)
    ratio = HQ // KVH
    query_blocks = queries.reshape(local_slots, BLOCK, local_heads, ratio, HD)
    scores = jnp.einsum(
        "sbgrd,scgd->sgrbc", query_blocks, key_blocks, preferred_element_type=jnp.float32
    ) * (1.0 / math.sqrt(HD))
    slot_lengths = lengths[my_seq]
    cached = jnp.arange(span, dtype=jnp.int32)
    allowed = (cached[None, None, :] <= query_pos[:, :, None]) & (
        cached[None, None, :] < slot_lengths[:, None, None]
    )
    scores = jnp.where(allowed[:, None, None], scores, -1e30)
    largest = jnp.max(scores, axis=-1, keepdims=True)
    weights = jnp.exp(scores - largest)
    probs = (weights / jnp.sum(weights, axis=-1, keepdims=True)).astype(jnp.bfloat16)
    mixed = jnp.einsum("sgrbc,scgd->sbgrd", probs, value_blocks, preferred_element_type=jnp.float32)
    valid = query_pos < slot_lengths[:, None]
    mixed = jnp.where(valid[:, :, None, None, None], mixed, 0.0)
    context = mixed.reshape(token_rows, local_heads * ratio * HD).astype(jnp.bfloat16)
    cache_rows = home_rows.reshape(span, 2 * head_width)
    own_length = lax.dynamic_slice_in_dim(lengths, replica, 1)[0]
    cache_rows = jnp.where((cached < own_length)[:, None], cache_rows, 0.0).astype(jnp.bfloat16)
    return (context, cache_rows[None, :, :head_width], cache_rows[None, :, head_width:])


MESH = pl.DeviceIdType.MESH
PIECES = 4
PAIR = 2
WRITES = 4
NEAR = (0, -1, 1)
UNITS = ((0, 2), (2, 6), (0, 4))


def when_all(conditions, action):
    live = [c for c in conditions if c is not None]
    if not live:
        action()
        return
    test = live[0]
    for c in live[1:]:
        test = jnp.logical_and(test, c)
    pl.when(test)(action)


def rebuild_kernel(
    depth,
    hidden_ref,
    wk_ref,
    wv_ref,
    q_ref,
    len_ref,
    seq_ref,
    pos_ref,
    ctx_out,
    key_out,
    value_out,
    hid,
    wt,
    acc,
    peer,
    xs,
    xr,
    kv0,
    kv1,
    kv2,
    kv3,
    sel,
    home_sel,
    arr0,
    arr1,
    home0,
    home1,
    qv,
    cos_t,
    sin_t,
    local_sem,
    send_sem,
    w_recv,
    h_recv,
    p_recv,
    x_recv,
    z_recv,
    u_recv,
):
    me = lax.axis_index("dp")
    core = lax.axis_index("mp")
    x = me % 2
    y = (me // 2) % 2
    z = me // 4
    mine = y * 2 + x
    rows = hidden_ref.shape[0]
    feats = hid.shape[2]
    wide = wk_ref.shape[0]
    kvs = (kv0, kv1, kv2, kv3)
    half = BLOCK // 2
    arrs = (arr0, arr1)
    homes = (home0, home1)
    slots = rows // BLOCK
    plane_slots = 4 * slots
    across = (z * 4 + y * 2 + (1 - x), core)
    along = (z * 4 + (1 - y) * 2 + x, core)
    diagonal = (z * 4 + (1 - y) * 2 + (1 - x), core)
    other = (me, 1 - core)
    targets = (across, along, diagonal)
    plane_ids = (y * 2 + 1 - x, (1 - y) * 2 + x, (1 - y) * 2 + 1 - x)
    my_feats = pl.ds(pl.multiple_of(x * feats, 128), feats)
    nbr_feats = pl.ds(pl.multiple_of((1 - x) * feats, 128), feats)
    sends = []

    def up():
        return z + 1 < depth

    def down():
        return z > 0

    def exists(dz):
        if dz == 0:
            return None
        return z + dz < depth if dz > 0 else z + dz >= 0

    def to_z(sign):
        return (me + 4 * sign, core)

    def remote(src, dst, sem, device):
        copy = pltpu.make_async_remote_copy(
            src_ref=src,
            dst_ref=dst,
            send_sem=send_sem.at[len(sends)],
            recv_sem=sem,
            device_id=device,
            device_id_type=MESH,
        )
        return copy

    def send(conditions, src, dst, sem, device):
        copy = remote(src, dst, sem, device)
        sends.append((conditions, copy))
        assert len(sends) <= send_sem.shape[0]
        when_all(conditions, copy.start)

    def arrived(conditions, dst, sem):
        copy = pltpu.make_async_remote_copy(
            src_ref=dst,
            dst_ref=dst,
            send_sem=send_sem.at[0],
            recv_sem=sem,
            device_id=across,
            device_id_type=MESH,
        )
        when_all(conditions, copy.wait_recv)

    def w_piece(zc, kv, side):
        half = x if side == 0 else 1 - x
        return wt.at[zc, pl.ds(pl.multiple_of(kv * 2 * wide + half * wide, wide), wide)]

    def w_sem(zc, kv, side):
        return w_recv.at[zc * 4 + kv * 2 + side]

    half_q = qv.shape[2]
    order = (1 - core, core)
    local = []
    for i, (src, dst) in enumerate(
        [
            (hidden_ref.at[:, my_feats], hid.at[mine]),
            (wk_ref.at[:, my_feats], w_piece(z, 0, 0)),
            (wv_ref.at[:, my_feats], w_piece(z, 1, 0)),
        ]
        + [
            (q_ref.at[:, pl.ds(pl.multiple_of(order[j] * half_q, 128), half_q)], qv.at[j])
            for j in range(2)
        ]
    ):
        copy = pltpu.make_async_copy(src, dst, local_sem.at[i])
        copy.start()
        local.append(copy)

    barrier = pltpu.get_barrier_semaphore()

    def greet(device):
        pl.semaphore_signal(barrier, inc=1, device_id=device, device_id_type=MESH)

    for device in (across, along, diagonal, other):
        greet(device)
    pl.when(down())(lambda: greet(to_z(-1)))
    pl.when(up())(lambda: greet(to_z(1)))
    inner = jnp.logical_and(down(), up())
    pl.when(inner)(lambda: pl.semaphore_wait(barrier, 6))
    pl.when(jnp.logical_not(inner))(lambda: pl.semaphore_wait(barrier, 5))

    weights = (wk_ref, wv_ref)
    for kv in range(2):
        send([up()], weights[kv].at[:, my_feats], w_piece(z, kv, 0), w_sem(z, kv, 0), to_z(1))
        send([down()], weights[kv].at[:, my_feats], w_piece(z, kv, 0), w_sem(z, kv, 0), to_z(-1))
        give = wt.at[z, pl.ds(pl.multiple_of(kv * 2 * wide + x * wide, wide), wide)]
        send([], weights[kv].at[:, nbr_feats], give, w_sem(z, kv, 1), across)
    step = rows // PIECES
    for p in range(PIECES):
        part = pl.ds(p * step, step)
        send([], hidden_ref.at[part, nbr_feats], hid.at[mine, part], h_recv.at[mine * PIECES + p], across)
        send([], hidden_ref.at[part, my_feats], hid.at[mine, part], h_recv.at[mine * PIECES + p], along)

    total_slots = base = seq_ref.shape[0]
    replicas = [z * 4 + i for i in plane_ids] + [me]
    wanted = []
    for r in replicas:
        wanted += [seq_ref[r * slots + s] for s in range(slots)] + [r]

    def scan(n, found):
        s, m = seq_ref[n], pos_ref[n]
        weight = jnp.where(m == 0, 1, jnp.where(m == 1, base, jnp.where(m == 2, base**2, base**3)))
        coded = n * weight
        return tuple(f + jnp.where(s == w, coded, 0) for f, w in zip(found, wanted))

    found = (0,) * len(wanted)
    for n in range(total_slots):
        found = scan(n, found)
    picks = []
    for t in range(4):
        codes = found[3 * t : 3 * t + 3]
        early = [(codes[s] // base**m) % base for s in range(slots) for m in range(MAXB - 1)]
        home = [(codes[slots] // base**m) % base for m in range(MAXB)]
        picks.append((early, home))

    def tables():
        lane = lax.broadcasted_iota(jnp.int32, (BLOCK, HD), 1)
        indices = (lane % (HD // 2)).astype(jnp.float32)
        frequency = jnp.exp(-(2.0 * indices / HD) * math.log(500000.0))
        row = lax.broadcasted_iota(jnp.int32, (BLOCK, HD), 0)
        for i in range(plane_slots):
            start = pos_ref[z * plane_slots + i] * BLOCK
            angles = (start + row).astype(jnp.float32) * frequency
            cos_t[pl.ds(i * BLOCK, BLOCK)] = jnp.cos(angles)
            sines = jnp.sin(angles)
            sin_t[pl.ds(i * BLOCK, BLOCK)] = jnp.where(lane < HD // 2, -sines, sines)

    pl.when(x == 0)(tables)

    def w_arrive(dz, side):
        zc = z + dz
        here = exists(dz)
        for kv in range(2):
            piece = w_piece(zc, kv, side)
            sem = w_sem(zc, kv, side)
            arrived([here], piece, sem)
            if dz == 0:
                send([up()], piece, piece, sem, to_z(1))
                send([down()], piece, piece, sem, to_z(-1))
            elif abs(dz) < depth - 1:
                sign = 1 if dz < 0 else -1
                send([here, up() if sign > 0 else down()], piece, piece, sem, to_z(sign))

    def h_forward(p):
        part = pl.ds(p * step, step)
        src = plane_ids[0]
        block = hid.at[src, part]
        arrived([], block, h_recv.at[src * PIECES + p])
        send([], block, block, h_recv.at[src * PIECES + p], along)

    w_arrive(0, 1)
    w_arrive(-1, 0)
    w_arrive(1, 0)
    h_forward(0)
    h_forward(1)
    w_arrive(-1, 1)
    w_arrive(1, 1)
    h_forward(2)
    h_forward(3)
    w_arrive(-2, 0)
    w_arrive(2, 0)
    for copy in local:
        copy.wait()
    for p in range(PIECES):
        for src in plane_ids[1:]:
            arrived([], hid.at[src, pl.ds(p * step, step)], h_recv.at[src * PIECES + p])

    def owner(dz):
        return (z + dz) // 2

    def multiply(dz):
        zc = z + dz

        def run():
            for i in range(4):
                block = lax.dot_general(
                    hid[i], wt[zc], (((1,), (1,)), ((), ())), preferred_element_type=jnp.float32
                )
                part = pl.ds(i * rows, rows)
                acc[zc, 0, part] = block[:, :HD]
                acc[zc, 1, part] = block[:, HD:]

        when_all([exists(dz)], run)
        send(
            [exists(dz), owner(dz) != core],
            acc.at[zc],
            peer.at[zc % 2],
            p_recv.at[zc % 2],
            other,
        )

    def reduce(dz):
        zc = z + dz
        k = zc % 2
        mine_here = [exists(dz), owner(dz) == core]
        arrived(mine_here, peer.at[k], p_recv.at[k])

        def body():
            xs[k] = (acc[zc, 1 - x] + peer[k, 1 - x]).astype(jnp.bfloat16)

        when_all(mine_here, body)
        send(mine_here, xs.at[k], xr.at[k], x_recv.at[k], across)

    def finish(dz):
        zc = z + dz
        k = zc % 2
        outer = 1 - ((zc + 1) // 2) % 2
        arrived([exists(dz), owner(dz) == core], xr.at[k], x_recv.at[k])
        for j in range(2):

            def body(j=j):
                def store(i, block):
                    for p in range(2):
                        kvs[2 * j + p][z * plane_slots + i] = block[p * half : (p + 1) * half].astype(
                            jnp.bfloat16
                        )

                for i in range(plane_slots):
                    part = pl.ds(i * BLOCK, BLOCK)
                    total = acc[zc, x, part] + peer[k, x, part] + xr[k, part].astype(jnp.float32)

                    def turn(total=total, part=part, i=i):
                        store(i, total * cos_t[part] + pltpu.roll(total, HD // 2, 1) * sin_t[part])

                    pl.when(x == 0)(turn)
                    pl.when(x != 0)(functools.partial(store, i, total))

            when_all([exists(dz), owner(dz) == core, outer == j], body)

    def kv_part(p, plane):
        return kvs[p].at[pl.ds(plane * plane_slots, plane_slots)], z_recv.at[p * depth + plane]

    def own_sends(p, conditions):
        block, sem = kv_part(p, z)
        send(conditions + [up()], block, block, sem, to_z(1))
        send(conditions + [down()], block, block, sem, to_z(-1))

    def relay(p, dz, condition):
        block, sem = kv_part(p, z + dz)
        sign = 1 if dz < 0 else -1
        conditions = [condition, exists(dz), up() if sign > 0 else down()]
        arrived(conditions, block, sem)
        send(conditions, block, block, sem, to_z(sign))

    def relays(p):
        low = z * 2 < depth
        high = jnp.logical_not(low)
        for near, dz in ((1, 1), (-1, 1), (1, 2)):
            relay(p, near * dz, low)
            relay(p, -near * dz, high)

    def last(p):
        for dz in range(1, depth):
            for sign in (1, -1):
                block, sem = kv_part(p, z - sign * dz)
                onward = up() if sign > 0 else down()
                arrived([exists(-sign * dz), jnp.logical_not(onward)], block, sem)

    def unit_sem(p, t, kind):
        return u_recv.at[(p * 3 + t) * 3 + kind]

    def part_rows(p):
        return pl.ds(p % 2 * half, half)

    def landing(p, src, kind):
        return (homes if kind == 2 else arrs)[p // 2].at[src, pl.ds(*UNITS[kind]), part_rows(p)]

    def give_own(p):
        for t in range(3):
            src = kvs[p].at[pl.ds(z * plane_slots + plane_ids[t] * slots, slots)]
            send([], src, landing(p, mine, 0), unit_sem(p, t, 0), targets[t])
        arrs[p // 2][mine, pl.ds(0, slots), part_rows(p)] = kvs[p][pl.ds(me * slots, slots)]

    def give_picked(p):
        kv, j, part = kvs[p], p // 2, part_rows(p)
        for kind, staged in ((1, sel), (2, home_sel)):
            for t in range(3):
                for u in range(UNITS[kind][1]):
                    staged[j, t, u, part] = kv[picks[t][kind - 1][u]]
                send([], staged.at[j, t, :, part], landing(p, mine, kind), unit_sem(p, t, kind), targets[t])
        for u in range(UNITS[1][1]):
            arrs[j][mine, UNITS[1][0] + u, part] = kv[picks[3][0][u]]
        for u in range(UNITS[2][1]):
            homes[j][mine, u, part] = kv[picks[3][1][u]]

    def units_arrive(j, sources, kinds):
        for p in (2 * j, 2 * j + 1):
            for t in sources:
                for kind in kinds:
                    arrived([], landing(p, plane_ids[t], kind), unit_sem(p, t, kind))

    ratio = half_q // (2 * HD)
    head_span = ratio * HD
    def attend(j, part):
        units_arrive(j, (1, 2) if part else (0,), (0, 1))
        head = 1 - y if part else y
        lax.fori_loop(0, slots, functools.partial(attend_head, j, head), 0)

    def attend_head(j, h, s, _):
        earlier = MAXB - 1
        q_pos = pos_ref[me * slots + s]
        length = len_ref[seq_ref[me * slots + s]]
        row = lax.broadcasted_iota(jnp.int32, (BLOCK, BLOCK), 0)
        col = lax.broadcasted_iota(jnp.int32, (BLOCK, BLOCK), 1)
        start = q_pos * BLOCK
        parts = [jnp.where((col <= row) & (start + col < length), 0.0, -1e30)]
        for m in range(earlier):
            parts.append(jnp.full((BLOCK, BLOCK), jnp.where(m < q_pos, 0.0, -1e30), jnp.float32))
        bias = jnp.concatenate(parts, axis=1)
        bias = jnp.concatenate([bias] * PAIR, axis=0)
        valid = (start + row) < length
        pieces = []
        for kv in range(2):
            own = arrs[j][2 * h + kv, s]
            rest = arrs[j][2 * h + kv, pl.ds(slots + s * earlier, earlier)]
            pieces.append(jnp.concatenate([own, rest.reshape(earlier * BLOCK, HD)], axis=0))
        keys, values = pieces
        part = pl.ds(pl.multiple_of(s * BLOCK, BLOCK), BLOCK)
        for r in range(0, ratio, PAIR):
            q = jnp.concatenate(
                [
                    qv[j, part, pl.ds(pl.multiple_of(h * head_span + (r + i) * HD, HD), HD)]
                    for i in range(PAIR)
                ],
                axis=0,
            )
            scores = lax.dot_general(
                q, keys, (((1,), (1,)), ((), ())), preferred_element_type=jnp.float32
            )
            scores = scores + bias
            largest = jnp.max(scores, axis=1, keepdims=True)
            exps = jnp.exp2((scores - largest) * (math.log2(math.e) / math.sqrt(HD)))
            scale = 1.0 / jnp.sum(exps, axis=1, keepdims=True)
            mixed = jnp.dot(exps.astype(jnp.bfloat16), values, preferred_element_type=jnp.float32)
            mixed = mixed * scale
            for i in range(PAIR):
                piece = jnp.where(valid, mixed[i * BLOCK : (i + 1) * BLOCK], 0.0)
                place = order[j] * half_q + h * head_span + (r + i) * HD
                ctx_out[part, pl.ds(pl.multiple_of(place, HD), HD)] = piece.astype(jnp.bfloat16)
        return 0

    def caches(j):
        units_arrive(j, range(3), (2,))
        length = len_ref[me]
        for m in range(MAXB):
            place = m * BLOCK + lax.broadcasted_iota(jnp.int32, (BLOCK, HD), 0)
            for h in range(2):
                column = pl.ds(pl.multiple_of((order[j] * 2 + h) * HD, HD), HD)
                for kv, out in ((0, key_out), (1, value_out)):
                    block = homes[j][2 * h + kv, m]
                    out[0, pl.ds(m * BLOCK, BLOCK), column] = jnp.where(
                        place < length, block, jnp.zeros_like(block)
                    )

    for dz in NEAR:
        multiply(dz)
    w_arrive(-2, 1)
    w_arrive(2, 1)
    for dz in NEAR:
        reduce(dz)
    multiply(-2)
    multiply(2)
    for dz in NEAR:
        finish(dz)
    for dz in (-2, 2):
        reduce(dz)
    for dz in (-2, 2):
        finish(dz)
    edge = jnp.logical_not(inner)
    own_sends(0, [])
    give_own(0)
    relays(0)
    own_sends(1, [])
    give_own(1)
    relays(1)
    w_arrive(-3, 0)
    w_arrive(3, 0)
    w_arrive(-3, 1)
    w_arrive(3, 1)
    for dz in (-3, 3):
        multiply(dz)
    for dz in (-3, 3):
        reduce(dz)
    for dz in (-3, 3):
        finish(dz)
    for p in (2, 3):
        own_sends(p, [edge])
        give_own(p)
    for p in (0, 1):
        last(p)
        give_picked(p)
    for p in (2, 3):
        own_sends(p, [inner])
        relays(p)
    attend(0, 0)
    last(2)
    give_picked(2)
    attend(0, 1)
    caches(0)
    last(3)
    give_picked(3)
    attend(1, 0)
    attend(1, 1)
    caches(1)
    for conditions, copy in sends:
        when_all(conditions, copy.wait_send)


def write_kernel(ctx_ref, key_ref, value_ref, ctx_out, key_out, value_out, sem):
    step = ctx_ref.shape[0] // WRITES
    pairs = [(ctx_ref.at[pl.ds(i * step, step)], ctx_out.at[pl.ds(i * step, step)]) for i in range(WRITES)]
    pairs += [(key_ref, key_out), (value_ref, value_out)]
    copies = [pltpu.make_async_copy(a, b, sem.at[i]) for i, (a, b) in enumerate(pairs)]
    for copy in copies:
        copy.start()
    for copy in copies:
        copy.wait()


def fast_shards(hidden, w_key, w_value, queries, lengths, seq_of_slot, pos_of_slot):
    depth = lax.axis_size("dp") // 4
    rows, features = hidden.shape
    wide = w_key.shape[1]
    slots = rows // BLOCK
    local_heads = wide * 4 * depth // HD // 2
    half = features // 2
    total = seq_of_slot.shape[0]
    plane = 4 * rows
    dma = pltpu.SemaphoreType.DMA
    anywhere = pl.BlockSpec(memory_space=pltpu.HBM)
    vmem = pl.BlockSpec(memory_space=pltpu.VMEM)
    smem = pl.BlockSpec(memory_space=pltpu.SMEM)
    bf16, f32 = jnp.bfloat16, jnp.float32
    cache = pltpu.VMEM((1, MAXB * BLOCK, local_heads * HD), bf16)
    half_q = queries.shape[1] // 2
    found = pl.pallas_call(
        functools.partial(rebuild_kernel, depth),
        out_shape=(pltpu.VMEM(queries.shape, bf16), cache, cache),
        in_specs=[anywhere] * 4 + [smem] * 3,
        out_specs=(vmem,) * 3,
        scratch_shapes=[
            pltpu.VMEM((4, rows, half), bf16),
            pltpu.VMEM((depth, 4 * wide, half), bf16),
            pltpu.VMEM((depth, 2, plane, HD), f32),
            pltpu.VMEM((2, 2, plane, HD), f32),
            pltpu.VMEM((2, plane, HD), bf16),
            pltpu.VMEM((2, plane, HD), bf16),
        ]
        + [pltpu.VMEM((total, BLOCK // 2, HD), bf16)] * 4
        + [
            pltpu.VMEM((2, 3, 6, BLOCK, HD), bf16),
            pltpu.VMEM((2, 3, 4, BLOCK, HD), bf16),
            pltpu.VMEM((4, 8, BLOCK, HD), bf16),
            pltpu.VMEM((4, 8, BLOCK, HD), bf16),
            pltpu.VMEM((4, 4, BLOCK, HD), bf16),
            pltpu.VMEM((4, 4, BLOCK, HD), bf16),
            pltpu.VMEM((2, rows, half_q), bf16),
            pltpu.VMEM((plane, HD), f32),
            pltpu.VMEM((plane, HD), f32),
            dma((5,)),
            dma((192,)),
            dma((4 * depth,)),
            dma((4 * PIECES,)),
            dma((2,)),
            dma((2,)),
            dma((4 * depth,)),
            dma((36,)),
        ],
        compiler_params=pltpu.CompilerParams(
            collective_id=0, has_side_effects=True, vmem_limit_bytes=62300 * 2**10
        ),
    )(hidden, w_key.T, w_value.T, queries, lengths, seq_of_slot, pos_of_slot)
    free = pl.BlockSpec(memory_space=pl.ANY)
    return pl.pallas_call(
        write_kernel,
        out_shape=tuple(jax.ShapeDtypeStruct(f.shape, f.dtype) for f in found),
        in_specs=[vmem] * 3,
        out_specs=(free,) * 3,
        scratch_shapes=[dma((2 + WRITES,))],
        compiler_params=pltpu.CompilerParams(vmem_limit_bytes=8 * 2**20),
    )(*found)


def suits(mesh):
    replicas, halves = mesh.shape["dp"], mesh.shape["mp"]
    return halves == 2 and replicas % 8 == 0 and KVH * HD == replicas * (HD // 2)


def solution(mesh):
    in_specs = (P("dp", "mp"), P("mp", "dp"), P("mp", "dp"), P("dp", "mp"), P(), P(), P())
    out_specs = (P("dp", "mp"), P("dp", None, "mp"), P("dp", None, "mp"))
    return jax.shard_map(fast_shards if suits(mesh) else shards, mesh=mesh, in_specs=in_specs, out_specs=out_specs, check_vma=False)
```

```python
import functools
import math

import jax
import jax.numpy as jnp
from jax import lax
from jax.experimental import pallas as pl
from jax.experimental.pallas import tpu as pltpu
from jax.sharding import PartitionSpec as P

HQ = 64
KVH = 8
HD = 128
BLOCK = 128
MAXB = 4


def rotate(field, positions):
    halfway = field.shape[-1] // 2
    indices = jnp.arange(halfway, dtype=jnp.float32)
    frequency = jnp.exp(-(2.0 * indices / field.shape[-1]) * math.log(500000.0))
    angles = positions[:, None] * frequency[None, :]
    cosines = jnp.cos(angles)[:, None, :]
    sines = jnp.sin(angles)[:, None, :]
    front = field[..., :halfway]
    back = field[..., halfway:]
    return jnp.concatenate(
        [front * cosines - back * sines, back * cosines + front * sines], axis=-1
    )


def shards(hidden, w_key, w_value, queries, lengths, seq_of_slot, pos_of_slot):
    replica = lax.axis_index("dp")
    token_rows = hidden.shape[0]
    local_slots = token_rows // BLOCK
    key_full, value_full = (
        lax.all_gather(w_key, "dp", axis=1, tiled=True),
        lax.all_gather(w_value, "dp", axis=1, tiled=True),
    )
    key_sum = jnp.dot(hidden, key_full, preferred_element_type=jnp.float32)
    value_sum = jnp.dot(hidden, value_full, preferred_element_type=jnp.float32)
    key_raw, value_raw = (
        lax.psum_scatter(key_sum, "mp", scatter_dimension=1, tiled=True),
        lax.psum_scatter(value_sum, "mp", scatter_dimension=1, tiled=True),
    )
    head_width = key_raw.shape[1]
    local_heads = head_width // HD
    my_seq = lax.dynamic_slice_in_dim(seq_of_slot, replica * local_slots, local_slots)
    my_pos = lax.dynamic_slice_in_dim(pos_of_slot, replica * local_slots, local_slots)
    offsets = jnp.arange(BLOCK, dtype=jnp.int32)
    query_pos = my_pos[:, None] * BLOCK + offsets[None, :]
    key_rows = rotate(
        key_raw.reshape(token_rows, local_heads, HD),
        query_pos.reshape(token_rows).astype(jnp.float32),
    )
    key_rows = key_rows.reshape(token_rows, head_width).astype(jnp.bfloat16)
    value_rows = value_raw.astype(jnp.bfloat16)
    payload = jnp.concatenate([key_rows, value_rows], axis=1).reshape(
        local_slots, BLOCK * 2 * head_width
    )
    blocks = jnp.arange(MAXB, dtype=jnp.int32)
    needed = (
        (seq_of_slot[None, None, :] == my_seq[:, None, None])
        & (pos_of_slot[None, None, :] == blocks[None, :, None])
        & (blocks[None, :, None] < my_pos[:, None, None])
    )
    owned = (seq_of_slot[None, :] == replica) & (pos_of_slot[None, :] == blocks[:, None])
    needed_pick = needed.astype(jnp.bfloat16)
    owned_pick = owned.astype(jnp.bfloat16)
    portion = lax.all_gather(payload, "dp", axis=0, tiled=True)
    earlier = jnp.einsum("smn,nx->smx", needed_pick, portion, preferred_element_type=jnp.float32)
    home_rows = jnp.dot(owned_pick, portion, preferred_element_type=jnp.float32)
    own_block = (blocks[None, :] == my_pos[:, None]).astype(jnp.float32)
    assembled = (earlier + own_block[:, :, None] * payload[:, None, :].astype(jnp.float32)).astype(
        jnp.bfloat16
    )
    span = MAXB * BLOCK
    assembled = assembled.reshape(local_slots, span, 2 * head_width)
    key_blocks = assembled[:, :, :head_width].reshape(local_slots, span, local_heads, HD)
    value_blocks = assembled[:, :, head_width:].reshape(local_slots, span, local_heads, HD)
    ratio = HQ // KVH
    query_blocks = queries.reshape(local_slots, BLOCK, local_heads, ratio, HD)
    scores = jnp.einsum(
        "sbgrd,scgd->sgrbc", query_blocks, key_blocks, preferred_element_type=jnp.float32
    ) * (1.0 / math.sqrt(HD))
    slot_lengths = lengths[my_seq]
    cached = jnp.arange(span, dtype=jnp.int32)
    allowed = (cached[None, None, :] <= query_pos[:, :, None]) & (
        cached[None, None, :] < slot_lengths[:, None, None]
    )
    scores = jnp.where(allowed[:, None, None], scores, -1e30)
    largest = jnp.max(scores, axis=-1, keepdims=True)
    weights = jnp.exp(scores - largest)
    probs = (weights / jnp.sum(weights, axis=-1, keepdims=True)).astype(jnp.bfloat16)
    mixed = jnp.einsum("sgrbc,scgd->sbgrd", probs, value_blocks, preferred_element_type=jnp.float32)
    valid = query_pos < slot_lengths[:, None]
    mixed = jnp.where(valid[:, :, None, None, None], mixed, 0.0)
    context = mixed.reshape(token_rows, local_heads * ratio * HD).astype(jnp.bfloat16)
    cache_rows = home_rows.reshape(span, 2 * head_width)
    own_length = lax.dynamic_slice_in_dim(lengths, replica, 1)[0]
    cache_rows = jnp.where((cached < own_length)[:, None], cache_rows, 0.0).astype(jnp.bfloat16)
    return (context, cache_rows[None, :, :head_width], cache_rows[None, :, head_width:])


MESH = pl.DeviceIdType.MESH
PIECES = 4
PAIR = 4
WRITES = 4
NEAR = (0, -1, 1)
UNITS = ((0, 2), (2, 6), (0, 4))


def when_all(conditions, action):
    live = [c for c in conditions if c is not None]
    if not live:
        action()
        return
    test = live[0]
    for c in live[1:]:
        test = jnp.logical_and(test, c)
    pl.when(test)(action)


def rebuild_kernel(
    depth,
    hidden_ref,
    wk_ref,
    wv_ref,
    q_ref,
    len_ref,
    seq_ref,
    pos_ref,
    ctx_out,
    key_out,
    value_out,
    hid,
    wt,
    acc,
    peer,
    xs,
    xr,
    kv0,
    kv1,
    kv2,
    kv3,
    sel,
    home_sel,
    arr0,
    arr1,
    home0,
    home1,
    qv,
    cos_t,
    sin_t,
    local_sem,
    send_sem,
    w_recv,
    h_recv,
    p_recv,
    x_recv,
    z_recv,
    u_recv,
):
    me = lax.axis_index("dp")
    core = lax.axis_index("mp")
    x = me % 2
    y = (me // 2) % 2
    z = me // 4
    mine = y * 2 + x
    rows = hidden_ref.shape[0]
    feats = hid.shape[2]
    wide = wk_ref.shape[0]
    kvs = (kv0, kv1, kv2, kv3)
    half = BLOCK // 2
    arrs = (arr0, arr1)
    homes = (home0, home1)
    slots = rows // BLOCK
    plane_slots = 4 * slots
    across = (z * 4 + y * 2 + (1 - x), core)
    along = (z * 4 + (1 - y) * 2 + x, core)
    diagonal = (z * 4 + (1 - y) * 2 + (1 - x), core)
    other = (me, 1 - core)
    targets = (across, along, diagonal)
    plane_ids = (y * 2 + 1 - x, (1 - y) * 2 + x, (1 - y) * 2 + 1 - x)
    my_feats = pl.ds(pl.multiple_of(x * feats, 128), feats)
    nbr_feats = pl.ds(pl.multiple_of((1 - x) * feats, 128), feats)
    sends = []

    def up():
        return z + 1 < depth

    def down():
        return z > 0

    def exists(dz):
        if dz == 0:
            return None
        return z + dz < depth if dz > 0 else z + dz >= 0

    def to_z(sign):
        return (me + 4 * sign, core)

    def remote(src, dst, sem, device):
        copy = pltpu.make_async_remote_copy(
            src_ref=src,
            dst_ref=dst,
            send_sem=send_sem.at[len(sends)],
            recv_sem=sem,
            device_id=device,
            device_id_type=MESH,
        )
        return copy

    def send(conditions, src, dst, sem, device):
        copy = remote(src, dst, sem, device)
        sends.append((conditions, copy))
        assert len(sends) <= send_sem.shape[0]
        when_all(conditions, copy.start)

    def arrived(conditions, dst, sem):
        copy = pltpu.make_async_remote_copy(
            src_ref=dst,
            dst_ref=dst,
            send_sem=send_sem.at[0],
            recv_sem=sem,
            device_id=across,
            device_id_type=MESH,
        )
        when_all(conditions, copy.wait_recv)

    def w_piece(zc, kv, side):
        half = x if side == 0 else 1 - x
        return wt.at[zc, pl.ds(pl.multiple_of(kv * 2 * wide + half * wide, wide), wide)]

    def w_sem(zc, kv, side):
        return w_recv.at[zc * 4 + kv * 2 + side]

    half_q = qv.shape[2]
    order = (1 - core, core)
    local = []
    for i, (src, dst) in enumerate(
        [
            (hidden_ref.at[:, my_feats], hid.at[mine]),
            (wk_ref.at[:, my_feats], w_piece(z, 0, 0)),
            (wv_ref.at[:, my_feats], w_piece(z, 1, 0)),
        ]
        + [
            (q_ref.at[:, pl.ds(pl.multiple_of(order[j] * half_q, 128), half_q)], qv.at[j])
            for j in range(2)
        ]
    ):
        copy = pltpu.make_async_copy(src, dst, local_sem.at[i])
        copy.start()
        local.append(copy)

    barrier = pltpu.get_barrier_semaphore()

    def greet(device):
        pl.semaphore_signal(barrier, inc=1, device_id=device, device_id_type=MESH)

    for device in (across, along, diagonal, other):
        greet(device)
    pl.when(down())(lambda: greet(to_z(-1)))
    pl.when(up())(lambda: greet(to_z(1)))
    inner = jnp.logical_and(down(), up())
    pl.when(inner)(lambda: pl.semaphore_wait(barrier, 6))
    pl.when(jnp.logical_not(inner))(lambda: pl.semaphore_wait(barrier, 5))

    weights = (wk_ref, wv_ref)
    for kv in range(2):
        send([up()], weights[kv].at[:, my_feats], w_piece(z, kv, 0), w_sem(z, kv, 0), to_z(1))
        send([down()], weights[kv].at[:, my_feats], w_piece(z, kv, 0), w_sem(z, kv, 0), to_z(-1))
        give = wt.at[z, pl.ds(pl.multiple_of(kv * 2 * wide + x * wide, wide), wide)]
        send([], weights[kv].at[:, nbr_feats], give, w_sem(z, kv, 1), across)
    step = rows // PIECES
    for p in range(PIECES):
        part = pl.ds(p * step, step)
        send([], hidden_ref.at[part, nbr_feats], hid.at[mine, part], h_recv.at[mine * PIECES + p], across)
        send([], hidden_ref.at[part, my_feats], hid.at[mine, part], h_recv.at[mine * PIECES + p], along)

    total_slots = base = seq_ref.shape[0]
    replicas = [z * 4 + i for i in plane_ids] + [me]
    wanted = []
    for r in replicas:
        wanted += [seq_ref[r * slots + s] for s in range(slots)] + [r]

    def scan(n, found):
        s, m = seq_ref[n], pos_ref[n]
        weight = jnp.where(m == 0, 1, jnp.where(m == 1, base, jnp.where(m == 2, base**2, base**3)))
        coded = n * weight
        return tuple(f + jnp.where(s == w, coded, 0) for f, w in zip(found, wanted))

    found = (0,) * len(wanted)
    for n in range(total_slots):
        found = scan(n, found)
    picks = []
    for t in range(4):
        codes = found[3 * t : 3 * t + 3]
        early = [(codes[s] // base**m) % base for s in range(slots) for m in range(MAXB - 1)]
        home = [(codes[slots] // base**m) % base for m in range(MAXB)]
        picks.append((early, home))

    def tables():
        lane = lax.broadcasted_iota(jnp.int32, (BLOCK, HD), 1)
        indices = (lane % (HD // 2)).astype(jnp.float32)
        frequency = jnp.exp(-(2.0 * indices / HD) * math.log(500000.0))
        row = lax.broadcasted_iota(jnp.int32, (BLOCK, HD), 0)
        for i in range(plane_slots):
            start = pos_ref[z * plane_slots + i] * BLOCK
            angles = (start + row).astype(jnp.float32) * frequency
            cos_t[pl.ds(i * BLOCK, BLOCK)] = jnp.cos(angles)
            sines = jnp.sin(angles)
            sin_t[pl.ds(i * BLOCK, BLOCK)] = jnp.where(lane < HD // 2, -sines, sines)

    pl.when(x == 0)(tables)

    def w_arrive(dz, side):
        zc = z + dz
        here = exists(dz)
        for kv in range(2):
            piece = w_piece(zc, kv, side)
            sem = w_sem(zc, kv, side)
            arrived([here], piece, sem)
            if dz == 0:
                send([up()], piece, piece, sem, to_z(1))
                send([down()], piece, piece, sem, to_z(-1))
            elif abs(dz) < depth - 1:
                sign = 1 if dz < 0 else -1
                send([here, up() if sign > 0 else down()], piece, piece, sem, to_z(sign))

    def h_forward(p):
        part = pl.ds(p * step, step)
        src = plane_ids[0]
        block = hid.at[src, part]
        arrived([], block, h_recv.at[src * PIECES + p])
        send([], block, block, h_recv.at[src * PIECES + p], along)

    w_arrive(0, 1)
    w_arrive(-1, 0)
    w_arrive(1, 0)
    h_forward(0)
    h_forward(1)
    w_arrive(-1, 1)
    w_arrive(1, 1)
    h_forward(2)
    h_forward(3)
    w_arrive(-2, 0)
    w_arrive(2, 0)
    for copy in local:
        copy.wait()
    for p in range(PIECES):
        for src in plane_ids[1:]:
            arrived([], hid.at[src, pl.ds(p * step, step)], h_recv.at[src * PIECES + p])

    def owner(dz):
        return (z + dz) // 2

    def multiply(dz):
        zc = z + dz

        def run():
            for i in range(4):
                block = lax.dot_general(
                    hid[i], wt[zc], (((1,), (1,)), ((), ())), preferred_element_type=jnp.float32
                )
                part = pl.ds(i * rows, rows)
                acc[zc, 0, part] = block[:, :HD]
                acc[zc, 1, part] = block[:, HD:]

        when_all([exists(dz)], run)
        send(
            [exists(dz), owner(dz) != core],
            acc.at[zc],
            peer.at[zc % 2],
            p_recv.at[zc % 2],
            other,
        )

    def reduce(dz):
        zc = z + dz
        k = zc % 2
        mine_here = [exists(dz), owner(dz) == core]
        arrived(mine_here, peer.at[k], p_recv.at[k])

        def body():
            xs[k] = (acc[zc, 1 - x] + peer[k, 1 - x]).astype(jnp.bfloat16)

        when_all(mine_here, body)
        send(mine_here, xs.at[k], xr.at[k], x_recv.at[k], across)

    def finish(dz):
        zc = z + dz
        k = zc % 2
        outer = 1 - ((zc + 1) // 2) % 2
        arrived([exists(dz), owner(dz) == core], xr.at[k], x_recv.at[k])
        for j in range(2):

            def body(j=j):
                def store(i, block):
                    for p in range(2):
                        kvs[2 * j + p][z * plane_slots + i] = block[p * half : (p + 1) * half].astype(
                            jnp.bfloat16
                        )

                for i in range(plane_slots):
                    part = pl.ds(i * BLOCK, BLOCK)
                    total = acc[zc, x, part] + peer[k, x, part] + xr[k, part].astype(jnp.float32)

                    def turn(total=total, part=part, i=i):
                        store(i, total * cos_t[part] + pltpu.roll(total, HD // 2, 1) * sin_t[part])

                    pl.when(x == 0)(turn)
                    pl.when(x != 0)(functools.partial(store, i, total))

            when_all([exists(dz), owner(dz) == core, outer == j], body)

    def kv_part(p, plane):
        return kvs[p].at[pl.ds(plane * plane_slots, plane_slots)], z_recv.at[p * depth + plane]

    def own_sends(p, conditions):
        block, sem = kv_part(p, z)
        send(conditions + [up()], block, block, sem, to_z(1))
        send(conditions + [down()], block, block, sem, to_z(-1))

    def relay(p, dz, condition):
        block, sem = kv_part(p, z + dz)
        sign = 1 if dz < 0 else -1
        conditions = [condition, exists(dz), up() if sign > 0 else down()]
        arrived(conditions, block, sem)
        send(conditions, block, block, sem, to_z(sign))

    def relays(p):
        low = z * 2 < depth
        high = jnp.logical_not(low)
        for near, dz in ((1, 1), (-1, 1), (1, 2)):
            relay(p, near * dz, low)
            relay(p, -near * dz, high)

    def last(p):
        for dz in range(1, depth):
            for sign in (1, -1):
                block, sem = kv_part(p, z - sign * dz)
                onward = up() if sign > 0 else down()
                arrived([exists(-sign * dz), jnp.logical_not(onward)], block, sem)

    def unit_sem(p, t, kind):
        return u_recv.at[(p * 3 + t) * 3 + kind]

    def part_rows(p):
        return pl.ds(p % 2 * half, half)

    def landing(p, src, kind):
        return (homes if kind == 2 else arrs)[p // 2].at[src, pl.ds(*UNITS[kind]), part_rows(p)]

    def give_own(p):
        for t in range(3):
            src = kvs[p].at[pl.ds(z * plane_slots + plane_ids[t] * slots, slots)]
            send([], src, landing(p, mine, 0), unit_sem(p, t, 0), targets[t])
        arrs[p // 2][mine, pl.ds(0, slots), part_rows(p)] = kvs[p][pl.ds(me * slots, slots)]

    def give_picked(p):
        kv, j, part = kvs[p], p // 2, part_rows(p)
        for kind, staged in ((1, sel), (2, home_sel)):
            for t in range(3):
                for u in range(UNITS[kind][1]):
                    staged[j, t, u, part] = kv[picks[t][kind - 1][u]]
                send([], staged.at[j, t, :, part], landing(p, mine, kind), unit_sem(p, t, kind), targets[t])
        for u in range(UNITS[1][1]):
            arrs[j][mine, UNITS[1][0] + u, part] = kv[picks[3][0][u]]
        for u in range(UNITS[2][1]):
            homes[j][mine, u, part] = kv[picks[3][1][u]]

    def units_arrive(j, sources, kinds):
        for p in (2 * j, 2 * j + 1):
            for t in sources:
                for kind in kinds:
                    arrived([], landing(p, plane_ids[t], kind), unit_sem(p, t, kind))

    ratio = half_q // (2 * HD)
    head_span = ratio * HD
    def attend(j, part):
        units_arrive(j, (1, 2) if part else (0,), (0, 1))
        head = 1 - y if part else y
        lax.fori_loop(0, slots, functools.partial(attend_head, j, head), 0)

    def attend_head(j, h, s, _):
        earlier = MAXB - 1
        q_pos = pos_ref[me * slots + s]
        length = len_ref[seq_ref[me * slots + s]]
        row = lax.broadcasted_iota(jnp.int32, (BLOCK, BLOCK), 0)
        col = lax.broadcasted_iota(jnp.int32, (BLOCK, BLOCK), 1)
        start = q_pos * BLOCK
        parts = [jnp.where((col <= row) & (start + col < length), 0.0, -1e30)]
        for m in range(earlier):
            parts.append(jnp.full((BLOCK, BLOCK), jnp.where(m < q_pos, 0.0, -1e30), jnp.float32))
        bias = jnp.concatenate(parts, axis=1)
        bias = jnp.concatenate([bias] * PAIR, axis=0)
        valid = (start + row) < length
        pieces = []
        for kv in range(2):
            own = arrs[j][2 * h + kv, s]
            rest = arrs[j][2 * h + kv, pl.ds(slots + s * earlier, earlier)]
            pieces.append(jnp.concatenate([own, rest.reshape(earlier * BLOCK, HD)], axis=0))
        keys, values = pieces
        part = pl.ds(pl.multiple_of(s * BLOCK, BLOCK), BLOCK)
        for r in range(0, ratio, PAIR):
            q = jnp.concatenate(
                [
                    qv[j, part, pl.ds(pl.multiple_of(h * head_span + (r + i) * HD, HD), HD)]
                    for i in range(PAIR)
                ],
                axis=0,
            )
            scores = lax.dot_general(
                q, keys, (((1,), (1,)), ((), ())), preferred_element_type=jnp.float32
            )
            scores = scores + bias
            largest = jnp.max(scores, axis=1, keepdims=True)
            exps = jnp.exp2((scores - largest) * (math.log2(math.e) / math.sqrt(HD)))
            scale = 1.0 / jnp.sum(exps, axis=1, keepdims=True)
            mixed = jnp.dot(exps.astype(jnp.bfloat16), values, preferred_element_type=jnp.float32)
            mixed = mixed * scale
            for i in range(PAIR):
                piece = jnp.where(valid, mixed[i * BLOCK : (i + 1) * BLOCK], 0.0)
                place = order[j] * half_q + h * head_span + (r + i) * HD
                ctx_out[part, pl.ds(pl.multiple_of(place, HD), HD)] = piece.astype(jnp.bfloat16)
        return 0

    def caches(j):
        units_arrive(j, range(3), (2,))
        length = len_ref[me]
        for m in range(MAXB):
            place = m * BLOCK + lax.broadcasted_iota(jnp.int32, (BLOCK, HD), 0)
            for h in range(2):
                column = pl.ds(pl.multiple_of((order[j] * 2 + h) * HD, HD), HD)
                for kv, out in ((0, key_out), (1, value_out)):
                    block = homes[j][2 * h + kv, m]
                    out[0, pl.ds(m * BLOCK, BLOCK), column] = jnp.where(
                        place < length, block, jnp.zeros_like(block)
                    )

    for dz in NEAR:
        multiply(dz)
    w_arrive(-2, 1)
    w_arrive(2, 1)
    for dz in NEAR:
        reduce(dz)
    multiply(-2)
    multiply(2)
    for dz in NEAR:
        finish(dz)
    for dz in (-2, 2):
        reduce(dz)
    for dz in (-2, 2):
        finish(dz)
    edge = jnp.logical_not(inner)
    own_sends(0, [])
    give_own(0)
    relays(0)
    own_sends(1, [])
    give_own(1)
    relays(1)
    w_arrive(-3, 0)
    w_arrive(3, 0)
    w_arrive(-3, 1)
    w_arrive(3, 1)
    for dz in (-3, 3):
        multiply(dz)
    for dz in (-3, 3):
        reduce(dz)
    for dz in (-3, 3):
        finish(dz)
    for p in (2, 3):
        own_sends(p, [edge])
        give_own(p)
    for p in (0, 1):
        last(p)
        give_picked(p)
    for p in (2, 3):
        own_sends(p, [inner])
        relays(p)
    attend(0, 0)
    last(2)
    give_picked(2)
    attend(0, 1)
    caches(0)
    last(3)
    give_picked(3)
    attend(1, 0)
    attend(1, 1)
    caches(1)
    for conditions, copy in sends:
        when_all(conditions, copy.wait_send)


def write_kernel(ctx_ref, key_ref, value_ref, ctx_out, key_out, value_out, sem):
    step = ctx_ref.shape[0] // WRITES
    pairs = [(ctx_ref.at[pl.ds(i * step, step)], ctx_out.at[pl.ds(i * step, step)]) for i in range(WRITES)]
    pairs += [(key_ref, key_out), (value_ref, value_out)]
    copies = [pltpu.make_async_copy(a, b, sem.at[i]) for i, (a, b) in enumerate(pairs)]
    for copy in copies:
        copy.start()
    for copy in copies:
        copy.wait()


def fast_shards(hidden, w_key, w_value, queries, lengths, seq_of_slot, pos_of_slot):
    depth = lax.axis_size("dp") // 4
    rows, features = hidden.shape
    wide = w_key.shape[1]
    slots = rows // BLOCK
    local_heads = wide * 4 * depth // HD // 2
    half = features // 2
    total = seq_of_slot.shape[0]
    plane = 4 * rows
    dma = pltpu.SemaphoreType.DMA
    anywhere = pl.BlockSpec(memory_space=pltpu.HBM)
    vmem = pl.BlockSpec(memory_space=pltpu.VMEM)
    smem = pl.BlockSpec(memory_space=pltpu.SMEM)
    bf16, f32 = jnp.bfloat16, jnp.float32
    cache = pltpu.VMEM((1, MAXB * BLOCK, local_heads * HD), bf16)
    half_q = queries.shape[1] // 2
    found = pl.pallas_call(
        functools.partial(rebuild_kernel, depth),
        out_shape=(pltpu.VMEM(queries.shape, bf16), cache, cache),
        in_specs=[anywhere] * 4 + [smem] * 3,
        out_specs=(vmem,) * 3,
        scratch_shapes=[
            pltpu.VMEM((4, rows, half), bf16),
            pltpu.VMEM((depth, 4 * wide, half), bf16),
            pltpu.VMEM((depth, 2, plane, HD), f32),
            pltpu.VMEM((2, 2, plane, HD), f32),
            pltpu.VMEM((2, plane, HD), bf16),
            pltpu.VMEM((2, plane, HD), bf16),
        ]
        + [pltpu.VMEM((total, BLOCK // 2, HD), bf16)] * 4
        + [
            pltpu.VMEM((2, 3, 6, BLOCK, HD), bf16),
            pltpu.VMEM((2, 3, 4, BLOCK, HD), bf16),
            pltpu.VMEM((4, 8, BLOCK, HD), bf16),
            pltpu.VMEM((4, 8, BLOCK, HD), bf16),
            pltpu.VMEM((4, 4, BLOCK, HD), bf16),
            pltpu.VMEM((4, 4, BLOCK, HD), bf16),
            pltpu.VMEM((2, rows, half_q), bf16),
            pltpu.VMEM((plane, HD), f32),
            pltpu.VMEM((plane, HD), f32),
            dma((5,)),
            dma((192,)),
            dma((4 * depth,)),
            dma((4 * PIECES,)),
            dma((2,)),
            dma((2,)),
            dma((4 * depth,)),
            dma((36,)),
        ],
        compiler_params=pltpu.CompilerParams(
            collective_id=0, has_side_effects=True, vmem_limit_bytes=62300 * 2**10
        ),
    )(hidden, w_key.T, w_value.T, queries, lengths, seq_of_slot, pos_of_slot)
    free = pl.BlockSpec(memory_space=pl.ANY)
    return pl.pallas_call(
        write_kernel,
        out_shape=tuple(jax.ShapeDtypeStruct(f.shape, f.dtype) for f in found),
        in_specs=[vmem] * 3,
        out_specs=(free,) * 3,
        scratch_shapes=[dma((2 + WRITES,))],
        compiler_params=pltpu.CompilerParams(vmem_limit_bytes=8 * 2**20),
    )(*found)


def suits(mesh):
    replicas, halves = mesh.shape["dp"], mesh.shape["mp"]
    return halves == 2 and replicas % 8 == 0 and KVH * HD == replicas * (HD // 2)


def solution(mesh):
    in_specs = (P("dp", "mp"), P("mp", "dp"), P("mp", "dp"), P("dp", "mp"), P(), P(), P())
    out_specs = (P("dp", "mp"), P("dp", None, "mp"), P("dp", None, "mp"))
    return jax.shard_map(fast_shards if suits(mesh) else shards, mesh=mesh, in_specs=in_specs, out_specs=out_specs, check_vma=False)
```
